256 devices in a mesh: section: 32 (over x, z_hi, core), tp: 8 (over z_lo, y).
Axes of the slice: x: 4, y: 4, z: 8 (z_hi: 4, z_lo: 2; z = z_hi * 2 + z_lo), core: 2. Of those that a mesh axis runs over, the one named last changes fastest.
Arguments:
- carried: bfloat16 [32, 256, 5120], P('section', 'tp'), may hold values from -6 to 6
- carried_segments: int32 [32, 256], P('section'), may hold values from 0 to 31, as said below
- fresh_batch: bfloat16 [2, 256, 5120], P(None, 'tp'), may hold values from -6 to 6
- fresh_segments: int32 [2, 256], replicated, may hold values from 0 to 31, as said below
- qkv_weight: bfloat16 [32, 5120, 3, 2048], P('section', None, None, 'tp'), may hold values from -3.354102 to 3.354102
- out_weight: bfloat16 [32, 2048, 5120], P('section', 'tp'), may hold values from -0.09375 to 0.09375
- norm_gain: bfloat16 [32, 2560], P('section'), may hold values from 0.099609375 to 1.8984375
Outputs:
- layer_outputs: bfloat16 [2, 32, 256, 5120], P(None, 'section', 'tp')
- shadow_outputs: bfloat16 [32, 256, 5120], P('section', 'tp')
The draws below stay inside these ranges and needn't reach their ends.
Inputs may be any that keep to these rules, and one draw needn't show every extreme that they name: `carried_segments`: document ids of each micro-batch's 512 tokens, read in token order across its two halves, start at 0, never fall, and rise by one at each document start; every micro-batch holds exactly 32 documents. `fresh_segments`: the same law for the entering micro-batch.
All inputs are finite; a program needn't handle non-finite values.
Results may differ from the reference program's by a relative error of at most 0.019.
Values may be sent and summed in bfloat16 or wider, within the bound.
A program may use at most 128 MiB of HBM per device.

```python
import jax
import jax.numpy as jnp
from jax import lax

D = 5120
HEADS = 32
HD = 128
TOK = 512
STEPS = 2
SECTIONS = 16
HALF = 256
N_TP = 8


def segment_ids(key, count):
    pieces = max(2, TOK // 16)
    keys = jax.random.split(key, count)
    orders = jax.vmap(lambda single: jax.random.permutation(single, TOK - 1))(keys)
    chosen = orders[:, :pieces - 1] + 1
    marks = jnp.zeros((count, TOK), jnp.int32)
    marks = marks.at[jnp.arange(count)[:, None], chosen].set(1)
    marks = marks.at[:, 0].set(1)
    return (jnp.cumsum(marks, axis=1) - 1).astype(jnp.int32)


def draw_carried_segments(key, part):
    return segment_ids(jax.random.fold_in(key, 21), SECTIONS).reshape(SECTIONS * 2, TOK // 2)


def draw_fresh_segments(key, part):
    return segment_ids(jax.random.fold_in(key, 22), 1).reshape(2, TOK // 2)


def draw_qkv_weight(key, part):
    columns = HEADS * HD // 2
    drawn = jax.random.truncated_normal(jax.random.fold_in(key, 11), -6.0, 6.0, (SECTIONS * 2, D, 3, columns), jnp.float32) * D ** (-0.5)
    return drawn.astype(jnp.bfloat16)


def levels(own_key, extent, cuts, smallest, high):
    loudness = 1.0
    for position, blocks in cuts:
        steps = jax.random.uniform(jax.random.fold_in(jax.random.fold_in(own_key, 6), position), (blocks,), jnp.float32, smallest / len(cuts), high / len(cuts))
        loudness = loudness * jnp.repeat(jnp.exp(steps), extent[position] // blocks).reshape((-1,) + (1,) * (len(extent) - 1 - position))
    return loudness


def normal_values(own_key, dims, spread, reach, cuts=(), held_as=jnp.bfloat16):
    level = levels(own_key, dims, cuts, -0.22, 0.18) if cuts else 1.0
    values = jax.random.normal(own_key, dims, jnp.float32) * spread * level
    return jnp.minimum(jnp.maximum(values, -reach), reach).astype(held_as)


def setup_inputs(seed: int = 0) -> dict:
    arg_keys = jax.random.split(jax.random.key(seed), 8)
    carried = normal_values(arg_keys[0], (2 * SECTIONS, HALF, D), 1.0, 6.0, ((0, 32), (1, 8)))
    carried_segments = draw_carried_segments(jax.random.fold_in(arg_keys[7], 71), 0)
    fresh_batch = normal_values(arg_keys[2], (2, HALF, D), 1.0, 6.0, ((1, 8),))
    fresh_segments = draw_fresh_segments(jax.random.fold_in(arg_keys[7], 71), 0)
    qkv_weight = draw_qkv_weight(jax.random.fold_in(arg_keys[7], 71), 0)
    out_weight = normal_values(arg_keys[5], (2 * SECTIONS, HEADS * HD // 2, D), (HEADS * HD) ** -0.5, 0.09375, ((0, 32), (1, 8)))
    norm_gain = jnp.clip(1.0 + 0.18 * jax.random.normal(arg_keys[6], (2 * SECTIONS, D // 2), jnp.float32), 0.099609375, 1.8984375).astype(jnp.bfloat16)
    return dict(carried=carried, carried_segments=carried_segments, fresh_batch=fresh_batch, fresh_segments=fresh_segments, qkv_weight=qkv_weight, out_weight=out_weight, norm_gain=norm_gain)


eps = 1e-05
rope_base = 10000.0

def normalize(values, gain):
    widened = values.astype(jnp.float32)
    power = lax.optimization_barrier(jnp.mean(widened * widened, axis=-1, keepdims=True))
    return (widened * lax.rsqrt(power + eps) * gain.astype(jnp.float32)).astype(jnp.bfloat16)

def rotate(values, positions):
    half_dim = values.shape[-1] // 2
    frequency = rope_base ** (-(jnp.arange(half_dim, dtype=jnp.float32) * 2.0 / values.shape[-1]))
    angles = positions.astype(jnp.float32)[:, None] * frequency[None, :]
    cosine = jnp.cos(angles)[:, None, :]
    sine = jnp.sin(angles)[:, None, :]
    leading = values[..., :half_dim]
    trailing = values[..., half_dim:]
    return jnp.concatenate([leading * cosine - trailing * sine, trailing * cosine + leading * sine], axis=-1)

def attend(projected, positions, segments):
    count = projected.shape[0]
    width = projected.shape[1] // 3
    parts = projected.reshape(count, 3, width // HD, HD)
    queries = rotate(parts[:, 0], positions).astype(jnp.bfloat16)
    keyed = rotate(parts[:, 1], positions).astype(jnp.bfloat16)
    values = parts[:, 2].astype(jnp.bfloat16)
    scores = jnp.einsum('qhd,khd->hqk', queries.astype(jnp.float32), keyed.astype(jnp.float32)) * HD ** (-0.5)
    visible = (positions[None, :] <= positions[:, None]) & (segments[None, :] == segments[:, None])
    masked = jnp.where(visible[None], scores, -1e+30)
    highest = lax.optimization_barrier(jnp.max(masked, axis=-1, keepdims=True))
    weights = jnp.where(visible[None], jnp.exp(masked - highest), 0.0)
    shares = (weights / lax.optimization_barrier(jnp.sum(weights, axis=-1, keepdims=True))).astype(jnp.bfloat16)
    mixed = jnp.einsum('hqk,khd->qhd', shares.astype(jnp.float32), values.astype(jnp.float32))
    return mixed.astype(jnp.bfloat16).reshape(count, width)

def layer(bundle):
    rows, segments, gain, weights_in, weights_out = bundle
    matrix = jnp.transpose(weights_in, (1, 2, 0, 3)).reshape(D, 3 * HEADS * HD)
    normed = normalize(rows, gain)
    projected = jnp.dot(normed, matrix, preferred_element_type=jnp.float32)
    positions = jnp.arange(TOK, dtype=jnp.int32)
    mixed = attend(projected, positions, segments)
    groups = 2 * N_TP
    width = HEADS * HD // groups
    blocks = mixed.reshape(TOK, groups, width).astype(jnp.float32)
    out_blocks = weights_out.reshape(groups, width, D).astype(jnp.float32)
    partials = jnp.einsum('tgc,gcd->gtd', blocks, out_blocks)
    rounded = lax.optimization_barrier(partials.astype(jnp.bfloat16)).astype(jnp.float32)
    return (rows.astype(jnp.float32) + lax.optimization_barrier(jnp.sum(rounded, axis=0))).astype(jnp.bfloat16)

def reference(carried, carried_segments, fresh_batch, fresh_segments, qkv_weight, out_weight, norm_gain):
    inputs_one = carried.reshape(SECTIONS, TOK, D)
    segments_one = carried_segments.reshape(SECTIONS, TOK)
    gains = norm_gain.reshape(SECTIONS, D)
    weights_in = qkv_weight.reshape(SECTIONS, 2, D, 3, HEADS * HD // 2)
    weights_out = out_weight.reshape(SECTIONS, HEADS * HD, D)
    outputs_one = lax.map(layer, (inputs_one, segments_one, gains, weights_in, weights_out))
    inputs_two = jnp.concatenate([fresh_batch.reshape(1, TOK, D), outputs_one[:-1]], axis=0)
    segments_two = jnp.concatenate([fresh_segments.reshape(1, TOK), segments_one[:-1]], axis=0)
    outputs_two = lax.map(layer, (inputs_two, segments_two, gains, weights_in, weights_out))
    shadow = jnp.concatenate([outputs_two[1:], jnp.zeros((1, TOK, D), jnp.bfloat16)], axis=0)
    stacked = jnp.stack([outputs_one, outputs_two]).reshape(STEPS, 2 * SECTIONS, HALF, D)
    return (stacked, shadow.reshape(2 * SECTIONS, HALF, D))
```

```python
import jax
import jax.numpy as jnp
import numpy as np
from jax import lax
from jax.experimental import pallas as pl
from jax.experimental.pallas import tpu as pltpu
from jax.sharding import PartitionSpec as P

HD = 128
EPS = 1e-05
ROPE_BASE = 10000.0
MASKED = -1e30
MESH = pl.DeviceIdType.MESH
CHUNKS = 4
CHUNK_GAP = 5.5
STEP_GAP = 4.0


def rope_tables(tokens):
    frequency = np.float32(ROPE_BASE) ** (-(np.arange(HD // 2, dtype=np.float32) * np.float32(2.0) / np.float32(HD)))
    angles = np.arange(tokens, dtype=np.float32)[:, None] * frequency.astype(np.float32)[None, :]
    cosine = np.cos(angles.astype(np.float64)).astype(np.float32)
    sine = np.sin(angles.astype(np.float64)).astype(np.float32)
    cosines = np.concatenate([cosine, cosine], axis=1)
    sines = np.concatenate([-sine, sine], axis=1)
    return np.stack([cosines, sines], axis=0)


def make_kernel(n_sections, width, block, heads_each):
    C = CHUNKS
    half = 8 * block
    cw = width // C
    gw = width // 2
    cols = heads_each * HD

    def kernel(
        carried, own_segments, fresh, fresh_segments, w_hbm, o_hbm, gain, tables,
        out, shadow,
        X, W, O, ACC, SS, XG, PB, RSA, RSB, RSZ, YS, SH, KV, KVO, MX, S, BIAS, G, SEGS, TAB,
        local_sem, send_sem, recv_sem,
    ):
        p = lax.axis_index("section")
        t = lax.axis_index("tp")
        core = lax.rem(p, 2)
        s = lax.div(p, 2)
        zl = lax.div(t, 4)
        y = lax.rem(t, 4)
        first = s == 0
        last = s == n_sections - 1

        def at(z, yy):
            return z * 4 + lax.rem(yy, 4)

        other_z = 1 - zl
        own, rz = t, at(other_z, y)
        up, down, far = at(zl, y + 1), at(zl, y + 3), at(zl, y + 2)
        z_up, z_down, z_far = at(other_z, y + 1), at(other_z, y + 3), at(other_z, y + 2)
        dev_z, dev_up, dev_down = (p, rz), (p, up), (p, down)
        partner = (p + 1 - 2 * core, t)
        ahead = (lax.rem(p + 2, 2 * n_sections), t)
        behind = (lax.rem(p + 2 * n_sections - 2, 2 * n_sections), t)

        def rows(b):
            return pl.ds(pl.multiple_of(b * block, block), block)

        def span(c):
            return pl.ds(c * cw, cw)

        counts = {"local": 0, "remote": 0}
        unsent = []

        def local_copy(src, dst):
            n = counts["local"]
            counts["local"] += 1
            return pltpu.make_async_copy(src, dst, local_sem.at[n])

        def message(src, dst, device):
            n = counts["remote"]
            counts["remote"] += 1
            copy = pltpu.make_async_remote_copy(
                src_ref=src, dst_ref=dst, send_sem=send_sem.at[n], recv_sem=recv_sem.at[n],
                device_id=device, device_id_type=MESH,
            )
            return copy

        def send(copy):
            copy.start()
            unsent.append(copy)

        own_rows = []
        for c in range(C):
            copy = local_copy(carried.at[0, :, span(c)], X.at[0, c, rows(own)])
            copy.start()
            own_rows.append(copy)
        w_own = []
        for c in range(C):
            copy = local_copy(w_hbm.at[:, span(c)], W.at[core, :, span(c)])
            copy.start()
            w_own.append(copy)
        o_own = local_copy(o_hbm.at[0], O.at[core])
        o_own.start()
        table_copy = local_copy(tables.at[:, pl.ds(pl.multiple_of(core * half, half), half)], TAB)
        table_copy.start()
        fresh_rows = [local_copy(fresh.at[core, :, span(c)], X.at[1, c, rows(own)]) for c in range(C)]

        @pl.when(first)
        def _():
            for copy in fresh_rows:
                copy.start()

        G[core] = jnp.broadcast_to(gain[...].astype(jnp.float32), (8, gw))
        SEGS[0, core] = jnp.broadcast_to(own_segments[...], (8, half))

        barrier = pltpu.get_barrier_semaphore()
        for device in (dev_z, dev_up, dev_down, partner, ahead, behind):
            pl.semaphore_signal(barrier, inc=1, device_id=device, device_id_type=MESH)
        pl.semaphore_wait(barrier, 6)

        ag = {}
        for l in range(2):
            for c in range(C):
                def block_of(b, device, l=l, c=c):
                    ref = X.at[l, c, rows(b)]
                    return message(ref, ref, device)
                ag[l, c] = dict(
                    z=block_of(own, dev_z),
                    down=block_of(own, dev_up),
                    up=block_of(own, dev_down),
                    z_down=block_of(rz, dev_up),
                    z_up=block_of(rz, dev_down),
                    far=block_of(down, dev_up) if c % 2 == 0 else block_of(up, dev_down),
                    z_far=block_of(far, dev_z),
                )

        def spread(l, c):
            for name in ("z", "down", "up"):
                send(ag[l, c][name])

        def relay(l, c):
            ag[l, c]["z"].wait_recv()
            send(ag[l, c]["z_down"])
            send(ag[l, c]["z_up"])
            ag[l, c]["down"].wait_recv()
            if c % 2 == 0:
                send(ag[l, c]["far"])
            ag[l, c]["up"].wait_recv()
            if c % 2 == 1:
                send(ag[l, c]["far"])

        def relay_far(l, c):
            ag[l, c]["far"].wait_recv()
            send(ag[l, c]["z_far"])

        def gathered(l, c):
            for name in ("z_down", "z_up", "z_far"):
                ag[l, c][name].wait_recv()

        for c in range(C):
            own_rows[c].wait()
            spread(0, c)
        w_other = []
        for c in range(C):
            copy = message(w_hbm.at[:, span(c)], W.at[core, :, span(c)], partner)
            send(copy)
            w_other.append(copy)
            if c == 0:
                gain_other = message(G.at[core], G.at[core], partner)
                send(gain_other)
                segments_other = message(SEGS.at[0, core], SEGS.at[0, core], partner)
                send(segments_other)
        o_other = message(o_hbm.at[0], O.at[core], partner)
        send(o_other)
        segments_ahead = message(SEGS.at[0], SEGS.at[1], ahead)

        def multiply(l, c):
            g0 = (c * cw) // gw
            scale = G[g0, 0:1, (c * cw) % gw:(c * cw) % gw + cw]

            def body(i, _):
                r = pl.ds(pl.multiple_of(i * 32, 32), 32)
                x = X[l, c, r].astype(jnp.float32)
                XG[r] = (x * scale).astype(jnp.bfloat16)
                square = x * x
                total = square[:, 0:HD]
                for k in range(1, cw // HD):
                    total = total + square[:, k * HD:(k + 1) * HD]
                if c == 0:
                    SS[r] = total
                else:
                    SS[r] = SS[r] + total
                return 0

            lax.fori_loop(0, half // 32, body, 0)
            for g in range(2):
                for j in range(3):
                    part = jnp.dot(XG[...], W[g, j, c * cw:(c + 1) * cw], preferred_element_type=jnp.float32)
                    if c == 0:
                        ACC[g, j] = part
                    else:
                        ACC[g, j] = ACC[g, j] + part

        def attend(l):
            power = jnp.sum(SS[...], axis=-1, keepdims=True) * (1.0 / width)
            factor = lax.rsqrt(power + EPS)
            heads = [(g, i) for g in range(2) for i in range(heads_each)]

            def rotated(v):
                return v * TAB[0] + pltpu.roll(v, HD // 2, 1) * TAB[1]

            for h, (g, i) in enumerate(heads):
                KV[l, 1, h] = (ACC[g, 2, :, i * HD:(i + 1) * HD] * factor).astype(jnp.bfloat16)
            values = message(KV.at[l, 1], KVO.at[l, 1], partner)
            send(values)
            for h, (g, i) in enumerate(heads):
                KV[l, 0, h] = rotated(ACC[g, 1, :, i * HD:(i + 1) * HD] * factor).astype(jnp.bfloat16)
            keys = message(KV.at[l, 0], KVO.at[l, 0], partner)
            send(keys)
            mine = jnp.broadcast_to(SEGS[l, core, 0:1], (HD, half)).astype(jnp.float32).T[:, 0:1]
            row_of = lax.broadcasted_iota(jnp.int32, (half, half), 0)
            column_of = lax.broadcasted_iota(jnp.int32, (half, half), 1)
            same = mine == SEGS[l, core, 0:1].astype(jnp.float32)
            BIAS[0] = jnp.where(same & (column_of <= row_of), 0.0, MASKED)
            elder = SEGS[l, 1 - core, 0:1].astype(jnp.float32)
            elder = jnp.where(core == 1, elder, -1.0)
            BIAS[1] = jnp.where(mine == elder, 0.0, MASKED)
            for h, (g, i) in enumerate(heads):
                q = rotated(ACC[g, 0, :, i * HD:(i + 1) * HD] * factor).astype(jnp.bfloat16)
                MX[:, h * HD:(h + 1) * HD] = q
                scores = lax.dot_general(q, KV[l, 0, h], (((1,), (1,)), ((), ())), preferred_element_type=jnp.float32)
                S[h] = scores * HD ** (-0.5) + BIAS[0]
            values.wait_recv()
            keys.wait_recv()
            for h in range(len(heads)):
                q = MX[:, h * HD:(h + 1) * HD]
                near = S[h]
                away = lax.dot_general(q, KVO[l, 0, h], (((1,), (1,)), ((), ())), preferred_element_type=jnp.float32)
                away = away * HD ** (-0.5) + BIAS[1]
                top = jnp.maximum(jnp.max(near, axis=-1, keepdims=True), jnp.max(away, axis=-1, keepdims=True))
                near = jnp.exp(near - top)
                away = jnp.exp(away - top)
                total = jnp.sum(near, axis=-1, keepdims=True) + jnp.sum(away, axis=-1, keepdims=True)
                mixed = jnp.dot(near.astype(jnp.bfloat16), KV[l, 1, h], preferred_element_type=jnp.float32)
                mixed = mixed + jnp.dot(away.astype(jnp.bfloat16), KVO[l, 1, h], preferred_element_type=jnp.float32)
                MX[:, h * HD:(h + 1) * HD] = (mixed / total).astype(jnp.bfloat16)

        rs = {}
        for l in range(2):
            for c in range(C):
                def part(b, ref, device, l=l, c=c):
                    return message(PB.at[l, c, rows(b)], ref, device)
                even = c % 2 == 0
                rs[l, c] = dict(
                    a0=part(far if even else z_far, RSA.at[l, c, 0], dev_up),
                    a1=part(z_far if even else far, RSA.at[l, c, 1], dev_down),
                    b0=part(up, RSB.at[l, c, 0], dev_up),
                    b1=part(down, RSB.at[l, c, 1], dev_down),
                    b2=part(z_up, RSB.at[l, c, 2], dev_up),
                    b3=part(z_down, RSB.at[l, c, 3], dev_down),
                    z=part(rz, RSZ.at[l, c], dev_z),
                )
        shifts = {}
        for c in range(C):
            shifts[0, c] = message(YS.at[0, c], X.at[1, c, rows(own)], ahead)
            shifts[1, c] = message(YS.at[1, c], SH.at[c], behind)

        def f32(v):
            return v.astype(jnp.float32)

        def project(l, c):
            PB[l, c] = jnp.dot(
                MX[...], O[:, :, c * cw:(c + 1) * cw].reshape(2 * cols, cw), preferred_element_type=jnp.float32
            ).astype(jnp.bfloat16)
            m = rs[l, c]
            for name in ("a0", "a1", "b2", "b1") if c % 2 == 0 else ("a0", "a1", "b0", "b3"):
                send(m[name])

        def fold_far(l, c):
            m = rs[l, c]
            m["a0"].wait_recv()
            m["a1"].wait_recv()
            even = c % 2 == 0
            for slot, b in ((0, up if even else z_up), (1, z_down if even else down)):
                r = rows(b)
                PB[l, c, r] = (f32(PB[l, c, r]) + f32(RSA[l, c, slot])).astype(jnp.bfloat16)
            for name in ("b3", "b0") if even else ("b2", "b1"):
                send(m[name])

        def fold_z(l, c):
            m = rs[l, c]
            m["b2"].wait_recv()
            m["b3"].wait_recv()
            r = rows(rz)
            PB[l, c, r] = (f32(PB[l, c, r]) + f32(RSB[l, c, 2]) + f32(RSB[l, c, 3])).astype(jnp.bfloat16)
            send(m["z"])

        def finish(l, c):
            m = rs[l, c]
            m["b0"].wait_recv()
            m["b1"].wait_recv()
            m["z"].wait_recv()
            r = rows(own)
            total = f32(PB[l, c, r]) + f32(RSB[l, c, 0]) + f32(RSB[l, c, 1]) + f32(RSZ[l, c])
            result = (f32(X[l, c, r]) + total).astype(jnp.bfloat16)
            YS[l, c] = result
            out[l, 0, :, c * cw:(c + 1) * cw] = result

            @pl.when(jnp.logical_not(last) if l == 0 else jnp.logical_not(first))
            def _():
                shifts[l, c].start()

        def enter(c):
            @pl.when(first)
            def _():
                fresh_rows[c].wait()

            @pl.when(jnp.logical_not(first))
            def _():
                shifts[0, c].wait_recv()

            spread(1, c)

        def leave(c):
            @pl.when(jnp.logical_not(last))
            def _():
                shifts[1, c].wait_recv()
                shadow[0, :, c * cw:(c + 1) * cw] = SH[c]

            @pl.when(last)
            def _():
                shadow[0, :, c * cw:(c + 1) * cw] = jnp.zeros((block, cw), jnp.bfloat16)

        def run(steps):
            order = sorted((c * CHUNK_GAP + k * STEP_GAP, c, k) for c in range(C) for k in range(len(steps)))
            for _, c, k in order:
                steps[k](c)

        for c in range(C):
            relay(0, c)
        gain_other.wait_recv()

        def compute_first(c):
            gathered(0, c)
            w_own[c].wait()
            w_other[c].wait_recv()
            multiply(0, c)

        for c in range(C):
            relay_far(0, c)
            if c >= 1:
                compute_first(c - 1)
        compute_first(C - 1)
        segments_other.wait_recv()

        @pl.when(jnp.logical_not(last))
        def _():
            segments_ahead.start()

        table_copy.wait()
        attend(0)
        o_own.wait()
        o_other.wait_recv()

        def compute_second(c):
            gathered(1, c)
            multiply(1, c)

        run([
            lambda c: project(0, c),
            lambda c: fold_far(0, c),
            lambda c: fold_z(0, c),
            lambda c: finish(0, c),
            enter,
            lambda c: relay(1, c),
            lambda c: relay_far(1, c),
            compute_second,
        ])

        @pl.when(first)
        def _():
            for b in range(2):
                SEGS[1, b] = jnp.broadcast_to(fresh_segments[b:b + 1], (8, half))

        @pl.when(jnp.logical_not(first))
        def _():
            segments_ahead.wait_recv()

        attend(1)
        run([
            lambda c: project(1, c),
            lambda c: fold_far(1, c),
            lambda c: fold_z(1, c),
            lambda c: finish(1, c),
            leave,
        ])
        for copy in unsent:
            copy.wait_send()

        @pl.when(jnp.logical_not(last))
        def _():
            segments_ahead.wait_send()
            for c in range(C):
                shifts[0, c].wait_send()

        @pl.when(jnp.logical_not(first))
        def _():
            for c in range(C):
                shifts[1, c].wait_send()

    bf, f4 = jnp.bfloat16, jnp.float32
    heads = 2 * heads_each
    scratch = [
        pltpu.VMEM((2, C, half, cw), bf),
        pltpu.VMEM((2, 3, width, cols), bf),
        pltpu.VMEM((2, cols, width), bf),
        pltpu.VMEM((2, 3, half, cols), f4),
        pltpu.VMEM((half, HD), f4),
        pltpu.VMEM((half, cw), bf),
        pltpu.VMEM((2, C, half, cw), bf),
        pltpu.VMEM((2, C, 2, block, cw), bf),
        pltpu.VMEM((2, C, 4, block, cw), bf),
        pltpu.VMEM((2, C, block, cw), bf),
        pltpu.VMEM((2, C, block, cw), bf),
        pltpu.VMEM((C, block, cw), bf),
        pltpu.VMEM((2, 2, heads, half, HD), bf),
        pltpu.VMEM((2, 2, heads, half, HD), bf),
        pltpu.VMEM((half, heads * HD), bf),
        pltpu.VMEM((heads, half, half), f4),
        pltpu.VMEM((2, half, half), f4),
        pltpu.VMEM((2, 8, gw), f4),
        pltpu.VMEM((2, 2, 8, half), jnp.int32),
        pltpu.VMEM((2, half, HD), f4),
        pltpu.SemaphoreType.DMA((3 * C + 2,)),
        pltpu.SemaphoreType.DMA((2 * (7 + 7 + 1) * C + 2 * 2 + C + 4,)),
        pltpu.SemaphoreType.DMA((2 * (7 + 7 + 1) * C + 2 * 2 + C + 4,)),
    ]
    return kernel, scratch


def per_device(carried, carried_segments, fresh_batch, fresh_segments, qkv_weight, out_weight, norm_gain):
    _, block, width = carried.shape
    cols = qkv_weight.shape[-1]
    n_sections = lax.axis_size("section") // 2
    kernel, scratch = make_kernel(n_sections, width, block, cols // HD)
    weights = jnp.transpose(qkv_weight[0], (1, 0, 2))
    tables = jnp.asarray(rope_tables(16 * block))
    vmem = pl.BlockSpec(memory_space=pltpu.VMEM)
    hbm = pl.BlockSpec(memory_space=pl.ANY)
    out, shadow = pl.pallas_call(
        kernel,
        name="relay",
        out_shape=(
            jax.ShapeDtypeStruct((2, 1, block, width), jnp.bfloat16),
            jax.ShapeDtypeStruct((1, block, width), jnp.bfloat16),
        ),
        in_specs=[hbm, vmem, hbm, vmem, hbm, hbm, vmem, hbm],
        out_specs=(vmem, vmem),
        scratch_shapes=scratch,
        compiler_params=pltpu.CompilerParams(
            collective_id=0, has_side_effects=True, vmem_limit_bytes=60 * 2**20
        ),
    )(carried, carried_segments, fresh_batch, fresh_segments, weights, out_weight, norm_gain, tables)
    return out, shadow


def solution(mesh):
    return jax.shard_map(
        per_device,
        mesh=mesh,
        in_specs=(
            P("section", "tp", None),
            P("section", None),
            P(None, "tp", None),
            P(),
            P("section", None, None, "tp"),
            P("section", "tp", None),
            P("section", None),
        ),
        out_specs=(P(None, "section", "tp", None), P("section", "tp", None)),
        check_vma=False,
    )
```

```python
import jax
import jax.numpy as jnp
import numpy as np
from jax import lax
from jax.experimental import pallas as pl
from jax.experimental.pallas import tpu as pltpu
from jax.sharding import PartitionSpec as P

HD = 128
EPS = 1e-05
ROPE_BASE = 10000.0
MASKED = -1e30
MESH = pl.DeviceIdType.MESH
CHUNKS = 10
FIRST_ORDER = (
    (4, 6), (4, 5), (4, 2), (4, 0), (4, 4), (4, 8), (4, 7), (4, 9), (6, 6), (5, 6),
    (6, 4), (4, 1), (6, 8), (4, 3), (6, 7), (6, 0), (6, 9), (7, 6), (6, 5), (5, 9),
    (7, 4), (6, 2), (6, 1), (7, 7), (6, 3), (5, 4), (5, 8), (5, 7), (7, 9), (7, 8),
    (7, 0), (5, 5), (8, 6), (7, 5), (7, 2), (5, 2), (7, 3), (8, 9), (5, 3), (7, 1),
    (5, 0), (5, 1), (8, 4), (8, 8), (8, 7), (8, 5), (8, 2), (8, 3), (8, 0), (8, 1),
)
MIDDLE_ORDER = (
    (0, 2), (0, 1), (0, 0), (1, 2), (1, 1), (1, 0), (0, 3), (0, 4), (2, 2), (2, 1),
    (0, 6), (2, 0), (1, 3), (3, 2), (1, 4), (0, 8), (3, 1), (3, 0), (1, 6), (2, 3),
    (0, 5), (4, 2), (0, 7), (2, 4), (4, 1), (2, 6), (3, 3), (1, 8), (3, 4), (1, 5),
    (1, 7), (0, 9), (4, 0), (2, 8), (2, 5), (6, 2), (3, 6), (2, 7), (1, 9), (4, 3),
    (5, 1), (5, 0), (3, 5), (2, 9), (3, 7), (4, 6), (6, 3), (3, 8), (4, 4), (6, 0),
    (3, 9), (6, 1), (7, 2), (4, 5), (5, 6), (7, 1), (4, 7), (6, 5), (5, 2), (4, 8),
    (7, 3), (6, 4), (6, 6), (5, 3), (4, 9), (6, 7), (6, 8), (5, 5), (7, 5), (5, 4),
    (7, 0), (7, 4), (8, 2), (6, 9), (7, 6), (5, 8), (5, 7), (8, 3), (5, 9), (7, 8),
    (7, 7), (8, 1), (8, 5), (7, 9), (8, 0), (8, 4), (8, 6), (8, 8), (8, 7), (8, 9),
)
LAST_ORDER = (
    (0, 1), (0, 4), (0, 0), (1, 1), (1, 4), (0, 7), (1, 0), (2, 1), (0, 3), (0, 2),
    (2, 4), (2, 0), (3, 1), (1, 7), (0, 6), (3, 4), (1, 3), (1, 2), (2, 7), (3, 0),
    (0, 8), (1, 6), (2, 3), (0, 5), (2, 2), (3, 7), (4, 1), (0, 9), (4, 4), (2, 6),
    (3, 3), (1, 8), (1, 5), (3, 2), (1, 9), (2, 8), (4, 7), (2, 5), (3, 6), (2, 9),
    (4, 0), (4, 3), (3, 8), (3, 5), (4, 6), (4, 2), (3, 9), (4, 8), (4, 5), (4, 9),
)


def rope_tables(tokens):
    frequency = np.float32(ROPE_BASE) ** (-(np.arange(HD // 2, dtype=np.float32) * np.float32(2.0) / np.float32(HD)))
    angles = np.arange(tokens, dtype=np.float32)[:, None] * frequency.astype(np.float32)[None, :]
    cosine = np.cos(angles.astype(np.float64)).astype(np.float32)
    sine = np.sin(angles.astype(np.float64)).astype(np.float32)
    cosines = np.concatenate([cosine, cosine], axis=1)
    sines = np.concatenate([-sine, sine], axis=1)
    return np.stack([cosines, sines], axis=0)


def make_kernel(n_sections, width, block, heads_each):
    C = CHUNKS
    half = 8 * block
    cw = width // C
    gw = width // 2
    cols = heads_each * HD

    def kernel(
        carried, own_segments, fresh, fresh_segments, w_hbm, o_hbm, gain, tables,
        out, shadow,
        X, W, O, ACC, SS, XG, PB, R, YS, SH, KV, KVO, MX, S, BIAS, G, SEGS, TAB,
        local_sem, send_sem, recv_sem,
    ):
        p = lax.axis_index("section")
        t = lax.axis_index("tp")
        core = lax.rem(p, 2)
        s = lax.div(p, 2)
        zl = lax.div(t, 4)
        y = lax.rem(t, 4)
        first = s == 0
        last = s == n_sections - 1

        def at(z, yy):
            return z * 4 + lax.rem(yy, 4)

        other_z = 1 - zl
        own, rz = t, at(other_z, y)
        up, down, far = at(zl, y + 1), at(zl, y + 3), at(zl, y + 2)
        z_up, z_down, z_far = at(other_z, y + 1), at(other_z, y + 3), at(other_z, y + 2)
        dev_z, dev_up, dev_down = (p, rz), (p, up), (p, down)
        partner = (p + 1 - 2 * core, t)
        ahead = (lax.rem(p + 2, 2 * n_sections), t)
        behind = (lax.rem(p + 2 * n_sections - 2, 2 * n_sections), t)

        def rows(b):
            return pl.ds(pl.multiple_of(b * block, block), block)

        def span(c):
            return pl.ds(c * cw, cw)

        counts = {"local": 0, "sent": 0, "received": 0}

        def fresh_sem(kind, sems):
            n = counts[kind]
            counts[kind] += 1
            return sems.at[n]

        def local_copy(src, dst):
            return pltpu.make_async_copy(src, dst, fresh_sem("local", local_sem))

        unsent_early = []

        def send_group():
            return fresh_sem("sent", send_sem)

        def arrival():
            return fresh_sem("received", recv_sem)

        def message(src, dst, device, sent, arrived):
            return pltpu.make_async_remote_copy(
                src_ref=src, dst_ref=dst, send_sem=sent, recv_sem=arrived,
                device_id=device, device_id_type=MESH,
            )

        def wait_for(ref, sem):
            pltpu.make_async_copy(ref, ref, sem).wait()

        own_rows = []
        for c in range(C):
            copy = local_copy(carried.at[0, :, span(c)], X.at[0, c, rows(own)])
            copy.start()
            own_rows.append(copy)
        w_own = local_copy(w_hbm, W.at[core])
        w_own.start()
        o_own = local_copy(o_hbm.at[0], O.at[core])
        o_own.start()
        table_copy = local_copy(tables.at[:, pl.ds(pl.multiple_of(core * half, half), half)], TAB)
        table_copy.start()
        fresh_sem_all = fresh_sem("local", local_sem)
        fresh_rows = [
            pltpu.make_async_copy(fresh.at[core, :, span(c)], X.at[1, c, rows(own)], fresh_sem_all) for c in range(C)
        ]

        @pl.when(first)
        def _():
            for copy in fresh_rows:
                copy.start()

        G[core] = jnp.broadcast_to(gain[...].astype(jnp.float32), (8, gw))
        SEGS[0, core] = jnp.broadcast_to(own_segments[...], (8, half))

        barrier = pltpu.get_barrier_semaphore()
        for device in (dev_z, dev_up, dev_down, partner, ahead, behind):
            pl.semaphore_signal(barrier, inc=1, device_id=device, device_id_type=MESH)
        with jax.named_scope("entry"):
            pl.semaphore_wait(barrier, 6)

        ag_sent = [send_group() for _ in range(2)]
        rs_sent = [send_group() for _ in range(2)]
        shift_sent = [send_group() for _ in range(2)]
        ag_sem = {(c, k): arrival() for c in range(C) for k in ("z", "y", "far", "rest")}
        rs_sem = {(c, k): arrival() for c in range(C) for k in ("far", "z", "own")}

        ag = {}
        for l in range(2):
            for c in range(C):
                def block_of(b, device, kind, l=l, c=c):
                    ref = X.at[l, c, rows(b)]
                    return message(ref, ref, device, ag_sent[l], ag_sem[c, kind])
                even = c % 2 == 0
                ag[l, c] = dict(
                    z=block_of(own, dev_z, "z"),
                    down=block_of(own, dev_up, "y" if even else "rest"),
                    up=block_of(own, dev_down, "rest" if even else "y"),
                    z_down=block_of(rz, dev_up, "rest"),
                    z_up=block_of(rz, dev_down, "rest"),
                    far=block_of(down, dev_up, "far") if even else block_of(up, dev_down, "far"),
                    z_far=block_of(far, dev_z, "rest"),
                )

        def spread(l, c):
            for name in ("z", "down", "up"):
                ag[l, c][name].start()

        def relay_z(l, c):
            wait_for(X.at[l, c, rows(rz)], ag_sem[c, "z"])
            ag[l, c]["z_down"].start()
            ag[l, c]["z_up"].start()

        def relay_y(l, c):
            wait_for(X.at[l, c, rows(down if c % 2 == 0 else up)], ag_sem[c, "y"])
            ag[l, c]["far"].start()

        def relay_far(l, c):
            wait_for(X.at[l, c, rows(far)], ag_sem[c, "far"])
            ag[l, c]["z_far"].start()

        def gathered(l, c):
            wait_for(X.at[l, c, pl.ds(0, 4 * block)], ag_sem[c, "rest"])

        def spread_first(c):
            own_rows[c].wait()
            spread(0, c)

        w_sent = send_group()
        w_sem = [arrival() for _ in range(C)]
        small_sent, small_sem = [send_group() for _ in range(4)], [arrival() for _ in range(4)]
        w_other = {}
        for c in (c for k, c in FIRST_ORDER if k == 8):
            w_other[c] = message(w_hbm.at[:, span(c)], W.at[core, :, span(c)], partner, w_sent, w_sem[c])
            w_other[c].start()
            if len(w_other) == 1:
                gain_other = message(G.at[core], G.at[core], partner, small_sent[0], small_sem[0])
                gain_other.start()
                segments_other = message(
                    SEGS.at[0, core], SEGS.at[0, core], partner, small_sent[1], small_sem[1]
                )
                segments_other.start()
        o_other = message(o_hbm.at[0], O.at[core], partner, small_sent[2], small_sem[2])
        o_other.start()
        segments_ahead = message(SEGS.at[0], SEGS.at[1], ahead, small_sent[3], small_sem[3])

        begun = set()

        def multiply(l, c):
            opening = l not in begun
            begun.add(l)
            g0 = (c * cw) // gw
            scale = G[g0, 0:1, (c * cw) % gw:(c * cw) % gw + cw]

            def body(i, _):
                r = pl.ds(pl.multiple_of(i * 32, 32), 32)
                x = X[l, c, r].astype(jnp.float32)
                XG[r] = (x * scale).astype(jnp.bfloat16)
                square = x * x
                total = square[:, 0:HD]
                for k in range(1, cw // HD):
                    total = total + square[:, k * HD:(k + 1) * HD]
                if opening:
                    SS[r] = total
                else:
                    SS[r] = SS[r] + total
                return 0

            lax.fori_loop(0, half // 32, body, 0)
            for g in range(2):
                for j in range(3):
                    part = jnp.dot(XG[...], W[g, j, c * cw:(c + 1) * cw], preferred_element_type=jnp.float32)
                    if opening:
                        ACC[g, j] = part
                    else:
                        ACC[g, j] = ACC[g, j] + part

        def attend(l):
            power = jnp.sum(SS[...], axis=-1, keepdims=True) * (1.0 / width)
            factor = lax.rsqrt(power + EPS)
            heads = [(g, i) for g in range(2) for i in range(heads_each)]

            def rotated(v):
                return v * TAB[0] + pltpu.roll(v, HD // 2, 1) * TAB[1]

            for h, (g, i) in enumerate(heads):
                KV[l, 1, h] = (ACC[g, 2, :, i * HD:(i + 1) * HD] * factor).astype(jnp.bfloat16)
            values = message(KV.at[l, 1], KVO.at[l, 1], partner, send_group(), arrival())
            keys = message(KV.at[l, 0], KVO.at[l, 0], partner, send_group(), arrival())

            @pl.when(core == 0)
            def _():
                values.start()

            for h, (g, i) in enumerate(heads):
                KV[l, 0, h] = rotated(ACC[g, 1, :, i * HD:(i + 1) * HD] * factor).astype(jnp.bfloat16)

            @pl.when(core == 0)
            def _():
                keys.start()

            unsent_early.append(values)
            unsent_early.append(keys)
            mine = jnp.broadcast_to(SEGS[l, core, 0:1], (HD, half)).astype(jnp.float32).T[:, 0:1]
            row_of = lax.broadcasted_iota(jnp.int32, (half, half), 0)
            column_of = lax.broadcasted_iota(jnp.int32, (half, half), 1)
            same = mine == SEGS[l, core, 0:1].astype(jnp.float32)
            BIAS[0] = jnp.where(same & (column_of <= row_of), 0.0, MASKED)

            @pl.when(core == 1)
            def _():
                BIAS[1] = jnp.where(mine == SEGS[l, 0, 0:1].astype(jnp.float32), 0.0, MASKED)

            for h, (g, i) in enumerate(heads):
                q = rotated(ACC[g, 0, :, i * HD:(i + 1) * HD] * factor).astype(jnp.bfloat16)
                MX[:, h * HD:(h + 1) * HD] = q
                scores = lax.dot_general(q, KV[l, 0, h], (((1,), (1,)), ((), ())), preferred_element_type=jnp.float32)
                S[h] = scores * HD ** (-0.5) + BIAS[0]

            def columns(h):
                return slice(h * HD, (h + 1) * HD)

            @pl.when(core == 0)
            def _():
                for h in range(len(heads)):
                    near = S[h]
                    near = jnp.exp(near - jnp.max(near, axis=-1, keepdims=True))
                    total = jnp.sum(near, axis=-1, keepdims=True)
                    mixed = jnp.dot(near.astype(jnp.bfloat16), KV[l, 1, h], preferred_element_type=jnp.float32)
                    MX[:, columns(h)] = (mixed / total).astype(jnp.bfloat16)

            @pl.when(core == 1)
            def _():
                with jax.named_scope("keys_wait"):
                    values.wait_recv()
                    keys.wait_recv()
                for h in range(len(heads)):
                    q = MX[:, columns(h)]
                    near = S[h]
                    away = lax.dot_general(
                        q, KVO[l, 0, h], (((1,), (1,)), ((), ())), preferred_element_type=jnp.float32
                    )
                    away = away * HD ** (-0.5) + BIAS[1]
                    top = jnp.maximum(jnp.max(near, axis=-1, keepdims=True), jnp.max(away, axis=-1, keepdims=True))
                    near = jnp.exp(near - top)
                    away = jnp.exp(away - top)
                    total = jnp.sum(near, axis=-1, keepdims=True) + jnp.sum(away, axis=-1, keepdims=True)
                    mixed = jnp.dot(near.astype(jnp.bfloat16), KV[l, 1, h], preferred_element_type=jnp.float32)
                    mixed = mixed + jnp.dot(away.astype(jnp.bfloat16), KVO[l, 1, h], preferred_element_type=jnp.float32)
                    MX[:, columns(h)] = (mixed / total).astype(jnp.bfloat16)

        rs = {}
        for l in range(2):
            for c in range(C):
                def part(b, slot, device, kind, l=l, c=c):
                    return message(PB.at[l, c, rows(b)], R.at[l, c, slot], device, rs_sent[l], rs_sem[c, kind])
                even = c % 2 == 0
                rs[l, c] = dict(
                    a0=part(far if even else z_far, 0, dev_up, "far"),
                    a1=part(z_far if even else far, 1, dev_down, "far"),
                    b2=part(z_up, 2, dev_up, "z"),
                    b3=part(z_down, 3, dev_down, "z"),
                    b0=part(up, 4, dev_up, "own"),
                    b1=part(down, 5, dev_down, "own"),
                    z=part(rz, 6, dev_z, "own"),
                )
        shift_sem = [[arrival() for _ in range(C)] for _ in range(2)]
        shifts = {}
        for c in range(C):
            shifts[0, c] = message(YS.at[0, c], X.at[1, c, rows(own)], ahead, shift_sent[0], shift_sem[0][c])
            shifts[1, c] = message(YS.at[1, c], SH.at[c], behind, shift_sent[1], shift_sem[1][c])

        def f32(v):
            return v.astype(jnp.float32)

        def project(l, c):
            PB[l, c] = jnp.dot(
                MX[...], O[:, :, c * cw:(c + 1) * cw].reshape(2 * cols, cw), preferred_element_type=jnp.float32
            ).astype(jnp.bfloat16)
            m = rs[l, c]
            for name in ("a0", "a1", "b2", "b1") if c % 2 == 0 else ("a0", "a1", "b0", "b3"):
                m[name].start()

        def fold_far(l, c):
            m = rs[l, c]
            wait_for(R.at[l, c, pl.ds(0, 2)], rs_sem[c, "far"])
            even = c % 2 == 0
            for slot, b in ((0, up if even else z_up), (1, z_down if even else down)):
                r = rows(b)
                PB[l, c, r] = (f32(PB[l, c, r]) + f32(R[l, c, slot])).astype(jnp.bfloat16)
            for name in ("b3", "b0") if even else ("b2", "b1"):
                m[name].start()

        def fold_z(l, c):
            m = rs[l, c]
            wait_for(R.at[l, c, pl.ds(2, 2)], rs_sem[c, "z"])
            r = rows(rz)
            PB[l, c, r] = (f32(PB[l, c, r]) + f32(R[l, c, 2]) + f32(R[l, c, 3])).astype(jnp.bfloat16)
            m["z"].start()

        def finish(l, c):
            wait_for(R.at[l, c, pl.ds(4, 3)], rs_sem[c, "own"])
            r = rows(own)
            total = f32(PB[l, c, r]) + f32(R[l, c, 4]) + f32(R[l, c, 5]) + f32(R[l, c, 6])
            result = (f32(X[l, c, r]) + total).astype(jnp.bfloat16)
            YS[l, c] = result
            out[l, 0, :, c * cw:(c + 1) * cw] = result

            @pl.when(jnp.logical_not(last) if l == 0 else jnp.logical_not(first))
            def _():
                shifts[l, c].start()

        entered = []

        def enter(c):
            @pl.when(first)
            def _():
                if not entered:
                    wait_for(YS.at[0], fresh_sem_all)

            @pl.when(jnp.logical_not(first))
            def _():
                shifts[0, c].wait_recv()

            entered.append(c)
            spread(1, c)

        def leave(c):
            @pl.when(jnp.logical_not(last))
            def _():
                shifts[1, c].wait_recv()
                shadow[0, :, c * cw:(c + 1) * cw] = SH[c]

            @pl.when(last)
            def _():
                shadow[0, :, c * cw:(c + 1) * cw] = jnp.zeros((block, cw), jnp.bfloat16)

        def run(steps, order):
            for k, c in order:
                with jax.named_scope(f"step{k}c{c}"):
                    steps[k](c)

        gain_waited = []

        def compute_first(c):
            gathered(0, c)
            if not gain_waited:
                gain_other.wait_recv()
                gain_waited.append(True)
                w_own.wait()
            w_other[c].wait_recv()
            multiply(0, c)

        run({
            4: spread_first,
            5: lambda c: relay_z(0, c),
            6: lambda c: relay_y(0, c),
            7: lambda c: relay_far(0, c),
            8: compute_first,
        }, FIRST_ORDER)
        segments_other.wait_recv()

        @pl.when(jnp.logical_not(last))
        def _():
            segments_ahead.start()

        table_copy.wait()
        with jax.named_scope("attend_first"):
            attend(0)
        o_own.wait()
        o_other.wait_recv()

        def compute_second(c):
            gathered(1, c)
            multiply(1, c)

        run({
            0: lambda c: project(0, c),
            1: lambda c: fold_far(0, c),
            2: lambda c: fold_z(0, c),
            3: lambda c: finish(0, c),
            4: enter,
            5: lambda c: relay_z(1, c),
            6: lambda c: relay_y(1, c),
            7: lambda c: relay_far(1, c),
            8: compute_second,
        }, MIDDLE_ORDER)

        @pl.when(first)
        def _():
            for b in range(2):
                SEGS[1, b] = jnp.broadcast_to(fresh_segments[b:b + 1], (8, half))

        @pl.when(jnp.logical_not(first))
        def _():
            segments_ahead.wait_recv()

        with jax.named_scope("attend_second"):
            attend(1)
        run({
            0: lambda c: project(1, c),
            1: lambda c: fold_far(1, c),
            2: lambda c: fold_z(1, c),
            3: lambda c: finish(1, c),
            4: leave,
        }, LAST_ORDER)
        with jax.named_scope("drain"):
            for l in range(2):
                wait_for(R.at[l], ag_sent[l])
                wait_for(R.at[l], rs_sent[l])
            wait_for(W.at[core], w_sent)
            for copy in (gain_other, segments_other, o_other):
                copy.wait_send()

        @pl.when(core == 0)
        def _():
            for copy in unsent_early:
                copy.wait_send()

        @pl.when(jnp.logical_not(last))
        def _():
            segments_ahead.wait_send()
            wait_for(YS.at[0], shift_sent[0])

        @pl.when(jnp.logical_not(first))
        def _():
            wait_for(YS.at[1], shift_sent[1])

    bf, f4 = jnp.bfloat16, jnp.float32
    heads = 2 * heads_each
    scratch = [
        pltpu.VMEM((2, C, half, cw), bf),
        pltpu.VMEM((2, 3, width, cols), bf),
        pltpu.VMEM((2, cols, width), bf),
        pltpu.VMEM((2, 3, half, cols), f4),
        pltpu.VMEM((half, HD), f4),
        pltpu.VMEM((half, cw), bf),
        pltpu.VMEM((2, C, half, cw), bf),
        pltpu.VMEM((2, C, 7, block, cw), bf),
        pltpu.VMEM((2, C, block, cw), bf),
        pltpu.VMEM((C, block, cw), bf),
        pltpu.VMEM((2, 2, heads, half, HD), bf),
        pltpu.VMEM((2, 2, heads, half, HD), bf),
        pltpu.VMEM((half, heads * HD), bf),
        pltpu.VMEM((heads, half, half), f4),
        pltpu.VMEM((2, half, half), f4),
        pltpu.VMEM((2, 8, gw), f4),
        pltpu.VMEM((2, 2, 8, half), jnp.int32),
        pltpu.VMEM((2, half, HD), f4),
        pltpu.SemaphoreType.DMA((C + 4,)),
        pltpu.SemaphoreType.DMA((6 + 1 + 4 + 4,)),
        pltpu.SemaphoreType.DMA(((4 + 3 + 2 + 1) * C + 4 + 4,)),
    ]
    return kernel, scratch


def per_device(carried, carried_segments, fresh_batch, fresh_segments, qkv_weight, out_weight, norm_gain):
    _, block, width = carried.shape
    cols = qkv_weight.shape[-1]
    n_sections = lax.axis_size("section") // 2
    kernel, scratch = make_kernel(n_sections, width, block, cols // HD)
    weights = jnp.transpose(qkv_weight[0], (1, 0, 2))
    tables = jnp.asarray(rope_tables(16 * block))
    vmem = pl.BlockSpec(memory_space=pltpu.VMEM)
    hbm = pl.BlockSpec(memory_space=pltpu.HBM)
    out, shadow = pl.pallas_call(
        kernel,
        name="relay",
        out_shape=(
            jax.ShapeDtypeStruct((2, 1, block, width), jnp.bfloat16),
            jax.ShapeDtypeStruct((1, block, width), jnp.bfloat16),
        ),
        in_specs=[hbm, vmem, hbm, vmem, hbm, hbm, vmem, hbm],
        out_specs=(vmem, vmem),
        scratch_shapes=scratch,
        compiler_params=pltpu.CompilerParams(
            collective_id=0, has_side_effects=True, vmem_limit_bytes=60 * 2**20
        ),
    )(carried, carried_segments, fresh_batch, fresh_segments, weights, out_weight, norm_gain, tables)
    return out, shadow


def solution(mesh):
    return jax.shard_map(
        per_device,
        mesh=mesh,
        in_specs=(
            P("section", "tp", None),
            P("section", None),
            P(None, "tp", None),
            P(),
            P("section", None, None, "tp"),
            P("section", "tp", None),
            P("section", None),
        ),
        out_specs=(P(None, "section", "tp", None), P("section", "tp", None)),
        check_vma=False,
    )
```

```python
import jax
import jax.numpy as jnp
import numpy as np
from jax import lax
from jax.experimental import pallas as pl
from jax.experimental.pallas import tpu as pltpu
from jax.sharding import PartitionSpec as P

HD = 128
EPS = 1e-05
ROPE_BASE = 10000.0
MASKED = -1e30
MESH = pl.DeviceIdType.MESH
CHUNKS = 10
FIRST_ORDER = (
    (4, 6), (4, 1), (4, 7), (4, 9), (4, 4), (4, 5), (6, 1), (4, 8), (4, 3), (6, 7),
    (4, 2), (6, 9), (4, 0), (6, 6), (5, 5), (6, 4), (6, 8), (7, 1), (6, 0), (6, 2),
    (5, 6), (6, 5), (6, 3), (7, 7), (5, 4), (5, 9), (7, 6), (7, 9), (5, 7), (7, 4),
    (5, 0), (7, 8), (7, 5), (5, 8), (7, 0), (5, 1), (5, 3), (8, 6), (7, 2), (8, 4),
    (7, 3), (5, 2), (8, 9), (8, 7), (8, 5), (8, 0), (8, 8), (8, 1), (8, 3), (8, 2),
)
MIDDLE_ORDER = (
    (0, 9), (0, 0), (0, 5), (0, 3), (1, 9), (0, 2), (1, 0), (9, 0), (1, 5), (1, 3),
    (9, 9), (0, 7), (9, 5), (9, 3), (0, 8), (2, 9), (1, 2), (2, 0), (2, 5), (2, 3),
    (0, 6), (3, 9), (0, 1), (0, 4), (3, 0), (3, 3), (1, 7), (1, 8), (9, 8), (3, 5),
    (1, 6), (2, 2), (9, 2), (4, 0), (1, 4), (1, 1), (9, 1), (2, 8), (9, 4), (4, 3),
    (9, 6), (2, 7), (4, 5), (3, 2), (2, 4), (5, 3), (2, 1), (5, 5), (2, 6), (9, 7),
    (6, 0), (3, 8), (4, 2), (3, 4), (6, 5), (6, 3), (3, 6), (3, 1), (3, 7), (4, 8),
    (4, 9), (5, 2), (4, 4), (6, 2), (4, 6), (6, 8), (7, 0), (5, 0), (6, 9), (7, 3),
    (4, 1), (6, 4), (7, 2), (4, 7), (7, 8), (6, 6), (5, 4), (7, 5), (5, 9), (6, 1),
    (6, 7), (7, 9), (5, 8), (8, 3), (7, 4), (5, 1), (7, 6), (8, 2), (5, 6), (8, 0),
    (7, 1), (7, 7), (5, 7), (8, 5), (8, 8), (8, 9), (8, 4), (8, 6), (8, 1), (8, 7),
)
LAST_ORDER = (
    (0, 5), (0, 6), (0, 9), (0, 0), (1, 5), (0, 3), (1, 9), (1, 6), (0, 2), (1, 0),
    (9, 5), (2, 5), (9, 6), (1, 3), (2, 6), (9, 3), (0, 1), (2, 9), (1, 2), (9, 0),
    (2, 0), (3, 5), (0, 4), (2, 3), (0, 7), (3, 6), (1, 1), (9, 2), (0, 8), (2, 2),
    (3, 0), (3, 3), (1, 4), (9, 9), (1, 7), (4, 5), (9, 4), (2, 1), (3, 2), (1, 8),
    (2, 4), (9, 1), (9, 7), (3, 9), (9, 8), (2, 7), (2, 8), (3, 1), (3, 4), (4, 6),
    (3, 8), (4, 3), (3, 7), (4, 9), (4, 2), (4, 8), (4, 1), (4, 0), (4, 4), (4, 7),
)


def rope_tables(tokens):
    frequency = np.float32(ROPE_BASE) ** (-(np.arange(HD // 2, dtype=np.float32) * np.float32(2.0) / np.float32(HD)))
    angles = np.arange(tokens, dtype=np.float32)[:, None] * frequency.astype(np.float32)[None, :]
    cosine = np.cos(angles.astype(np.float64)).astype(np.float32)
    sine = np.sin(angles.astype(np.float64)).astype(np.float32)
    cosines = np.concatenate([cosine, cosine], axis=1)
    sines = np.concatenate([-sine, sine], axis=1)
    return np.stack([cosines, sines], axis=0)


def make_kernel(n_sections, width, block, heads_each):
    C = CHUNKS
    half = 8 * block
    cw = width // C
    gw = width // 2
    cols = heads_each * HD

    def kernel(
        carried, own_segments, fresh, fresh_segments, w_hbm, o_hbm, gain, tables,
        out, shadow,
        X, W, O, ACC, SS, XG, PB, R, YS, SH, KV, KVO, MX, S, BIAS, G, SEGS, TAB, GIN, SIN, FIN,
        local_sem, send_sem, recv_sem, out_sem,
    ):
        p = lax.axis_index("section")
        t = lax.axis_index("tp")
        core = lax.rem(p, 2)
        s = lax.div(p, 2)
        zl = lax.div(t, 4)
        y = lax.rem(t, 4)
        first = s == 0
        last = s == n_sections - 1

        def at(z, yy):
            return z * 4 + lax.rem(yy, 4)

        other_z = 1 - zl
        own, rz = t, at(other_z, y)
        up, down, far = at(zl, y + 1), at(zl, y + 3), at(zl, y + 2)
        z_up, z_down, z_far = at(other_z, y + 1), at(other_z, y + 3), at(other_z, y + 2)
        dev_z, dev_up, dev_down = (p, rz), (p, up), (p, down)
        partner = (p + 1 - 2 * core, t)
        ahead = (lax.rem(p + 2, 2 * n_sections), t)
        behind = (lax.rem(p + 2 * n_sections - 2, 2 * n_sections), t)

        def rows(b):
            return pl.ds(pl.multiple_of(b * block, block), block)

        def span(c):
            return pl.ds(c * cw, cw)

        counts = {"local": 0, "sent": 0, "received": 0}

        def fresh_sem(kind, sems):
            n = counts[kind]
            counts[kind] += 1
            return sems.at[n]

        def local_copy(src, dst):
            return pltpu.make_async_copy(src, dst, fresh_sem("local", local_sem))

        unsent_early = []

        def send_group():
            return fresh_sem("sent", send_sem)

        def arrival():
            return fresh_sem("received", recv_sem)

        def message(src, dst, device, sent, arrived):
            return pltpu.make_async_remote_copy(
                src_ref=src, dst_ref=dst, send_sem=sent, recv_sem=arrived,
                device_id=device, device_id_type=MESH,
            )

        def wait_for(ref, sem):
            pltpu.make_async_copy(ref, ref, sem).wait()

        small_loads = [local_copy(gain, GIN), local_copy(own_segments, SIN), local_copy(fresh_segments, FIN)]
        for copy in small_loads:
            copy.start()
        own_rows = []
        for c in range(C):
            copy = local_copy(carried.at[0, :, span(c)], X.at[0, c, rows(own)])
            copy.start()
            own_rows.append(copy)
        w_own = local_copy(w_hbm, W.at[core])
        w_own.start()
        o_own = local_copy(o_hbm.at[0], O.at[core])
        o_own.start()
        table_copy = local_copy(tables.at[:, pl.ds(pl.multiple_of(core * half, half), half)], TAB)
        table_copy.start()
        fresh_sem_all = fresh_sem("local", local_sem)
        fresh_rows = [
            pltpu.make_async_copy(fresh.at[core, :, span(c)], X.at[1, c, rows(own)], fresh_sem_all) for c in range(C)
        ]

        @pl.when(last)
        def _():
            SH[...] = jnp.zeros(SH.shape, SH.dtype)

        @pl.when(first)
        def _():
            for copy in fresh_rows:
                copy.start()

        barrier = pltpu.get_barrier_semaphore()
        for device in (dev_z, dev_up, dev_down, partner, ahead, behind):
            pl.semaphore_signal(barrier, inc=1, device_id=device, device_id_type=MESH)
        with jax.named_scope("entry"):
            pl.semaphore_wait(barrier, 6)
        for copy in small_loads:
            copy.wait()
        G[core] = jnp.broadcast_to(GIN[...].astype(jnp.float32), (8, gw))
        SEGS[0, core] = jnp.broadcast_to(SIN[...], (8, half))

        ag_sent = [send_group() for _ in range(2)]
        rs_sent = [send_group() for _ in range(2)]
        shift_sent = [send_group() for _ in range(2)]
        ag_sem = {(c, k): arrival() for c in range(C) for k in ("z", "y", "far", "rest")}
        rs_sem = {(c, k): arrival() for c in range(C) for k in ("far", "z", "own")}

        ag = {}
        for l in range(2):
            for c in range(C):
                def block_of(b, device, kind, l=l, c=c):
                    ref = X.at[l, c, rows(b)]
                    return message(ref, ref, device, ag_sent[l], ag_sem[c, kind])
                even = c % 2 == 0
                ag[l, c] = dict(
                    z=block_of(own, dev_z, "z"),
                    down=block_of(own, dev_up, "y" if even else "rest"),
                    up=block_of(own, dev_down, "rest" if even else "y"),
                    z_down=block_of(rz, dev_up, "rest"),
                    z_up=block_of(rz, dev_down, "rest"),
                    far=block_of(down, dev_up, "far") if even else block_of(up, dev_down, "far"),
                    z_far=block_of(far, dev_z, "rest"),
                )

        def spread(l, c):
            for name in ("z", "down", "up"):
                ag[l, c][name].start()

        def relay_z(l, c):
            wait_for(X.at[l, c, rows(rz)], ag_sem[c, "z"])
            ag[l, c]["z_down"].start()
            ag[l, c]["z_up"].start()

        def relay_y(l, c):
            wait_for(X.at[l, c, rows(down if c % 2 == 0 else up)], ag_sem[c, "y"])
            ag[l, c]["far"].start()

        def relay_far(l, c):
            wait_for(X.at[l, c, rows(far)], ag_sem[c, "far"])
            ag[l, c]["z_far"].start()

        def gathered(l, c):
            wait_for(X.at[l, c, pl.ds(0, 4 * block)], ag_sem[c, "rest"])

        def spread_first(c):
            own_rows[c].wait()
            spread(0, c)

        w_sent = send_group()
        w_sem = [arrival() for _ in range(C)]
        small_sent, small_sem = [send_group() for _ in range(4)], [arrival() for _ in range(4)]
        w_other = {}
        for c in (c for k, c in FIRST_ORDER if k == 8):
            w_other[c] = message(w_hbm.at[:, span(c)], W.at[core, :, span(c)], partner, w_sent, w_sem[c])
            w_other[c].start()
            if len(w_other) == 1:
                gain_other = message(G.at[core], G.at[core], partner, small_sent[0], small_sem[0])
                gain_other.start()
                segments_other = message(
                    SEGS.at[0, core], SEGS.at[0, core], partner, small_sent[1], small_sem[1]
                )
                segments_other.start()
        o_other = message(o_hbm.at[0], O.at[core], partner, small_sent[2], small_sem[2])
        o_other.start()
        segments_ahead = message(SEGS.at[0], SEGS.at[1], ahead, small_sent[3], small_sem[3])

        begun = set()

        def multiply(l, c):
            opening = l not in begun
            begun.add(l)
            g0 = (c * cw) // gw
            scale = G[g0, 0:1, (c * cw) % gw:(c * cw) % gw + cw]

            def body(i, _):
                r = pl.ds(pl.multiple_of(i * 32, 32), 32)
                x = X[l, c, r].astype(jnp.float32)
                XG[r] = (x * scale).astype(jnp.bfloat16)
                square = x * x
                total = square[:, 0:HD]
                for k in range(1, cw // HD):
                    total = total + square[:, k * HD:(k + 1) * HD]
                if opening:
                    SS[r] = total
                else:
                    SS[r] = SS[r] + total
                return 0

            lax.fori_loop(0, half // 32, body, 0)
            for g in range(2):
                for j in range(3):
                    part = jnp.dot(XG[...], W[g, j, c * cw:(c + 1) * cw], preferred_element_type=jnp.float32)
                    if opening:
                        ACC[g, j] = part
                    else:
                        ACC[g, j] = ACC[g, j] + part

        def attend(l):
            power = jnp.sum(SS[...], axis=-1, keepdims=True) * (1.0 / width)
            factor = lax.rsqrt(power + EPS)
            heads = [(g, i) for g in range(2) for i in range(heads_each)]

            def rotated(v):
                return v * TAB[0] + pltpu.roll(v, HD // 2, 1) * TAB[1]

            for h, (g, i) in enumerate(heads):
                KV[l, 1, h] = (ACC[g, 2, :, i * HD:(i + 1) * HD] * factor).astype(jnp.bfloat16)
            values = message(KV.at[l, 1], KVO.at[l, 1], partner, send_group(), arrival())
            keys = message(KV.at[l, 0], KVO.at[l, 0], partner, send_group(), arrival())

            @pl.when(core == 0)
            def _():
                values.start()

            for h, (g, i) in enumerate(heads):
                KV[l, 0, h] = rotated(ACC[g, 1, :, i * HD:(i + 1) * HD] * factor).astype(jnp.bfloat16)

            @pl.when(core == 0)
            def _():
                keys.start()

            unsent_early.append(values)
            unsent_early.append(keys)
            mine = jnp.broadcast_to(SEGS[l, core, 0:1], (HD, half)).astype(jnp.float32).T[:, 0:1]
            row_of = lax.broadcasted_iota(jnp.int32, (half, half), 0)
            column_of = lax.broadcasted_iota(jnp.int32, (half, half), 1)
            same = mine == SEGS[l, core, 0:1].astype(jnp.float32)
            BIAS[0] = jnp.where(same & (column_of <= row_of), 0.0, MASKED)

            @pl.when(core == 1)
            def _():
                BIAS[1] = jnp.where(mine == SEGS[l, 0, 0:1].astype(jnp.float32), 0.0, MASKED)

            for h, (g, i) in enumerate(heads):
                q = rotated(ACC[g, 0, :, i * HD:(i + 1) * HD] * factor).astype(jnp.bfloat16)
                MX[:, h * HD:(h + 1) * HD] = q
                scores = lax.dot_general(q, KV[l, 0, h], (((1,), (1,)), ((), ())), preferred_element_type=jnp.float32)
                S[h] = scores * HD ** (-0.5) + BIAS[0]

            def columns(h):
                return slice(h * HD, (h + 1) * HD)

            @pl.when(core == 0)
            def _():
                for h in range(len(heads)):
                    near = S[h]
                    near = jnp.exp(near - jnp.max(near, axis=-1, keepdims=True))
                    total = jnp.sum(near, axis=-1, keepdims=True)
                    mixed = jnp.dot(near.astype(jnp.bfloat16), KV[l, 1, h], preferred_element_type=jnp.float32)
                    MX[:, columns(h)] = (mixed / total).astype(jnp.bfloat16)

            @pl.when(core == 1)
            def _():
                with jax.named_scope("keys_wait"):
                    values.wait_recv()
                    keys.wait_recv()
                for h in range(len(heads)):
                    q = MX[:, columns(h)]
                    near = S[h]
                    away = lax.dot_general(
                        q, KVO[l, 0, h], (((1,), (1,)), ((), ())), preferred_element_type=jnp.float32
                    )
                    away = away * HD ** (-0.5) + BIAS[1]
                    top = jnp.maximum(jnp.max(near, axis=-1, keepdims=True), jnp.max(away, axis=-1, keepdims=True))
                    near = jnp.exp(near - top)
                    away = jnp.exp(away - top)
                    total = jnp.sum(near, axis=-1, keepdims=True) + jnp.sum(away, axis=-1, keepdims=True)
                    mixed = jnp.dot(near.astype(jnp.bfloat16), KV[l, 1, h], preferred_element_type=jnp.float32)
                    mixed = mixed + jnp.dot(away.astype(jnp.bfloat16), KVO[l, 1, h], preferred_element_type=jnp.float32)
                    MX[:, columns(h)] = (mixed / total).astype(jnp.bfloat16)

        rs = {}
        for l in range(2):
            for c in range(C):
                def part(b, slot, device, kind, l=l, c=c):
                    return message(PB.at[l, c, rows(b)], R.at[l, c, slot], device, rs_sent[l], rs_sem[c, kind])
                even = c % 2 == 0
                rs[l, c] = dict(
                    a0=part(far if even else z_far, 0, dev_up, "far"),
                    a1=part(z_far if even else far, 1, dev_down, "far"),
                    b2=part(z_up, 2, dev_up, "z"),
                    b3=part(z_down, 3, dev_down, "z"),
                    b0=part(up, 4, dev_up, "own"),
                    b1=part(down, 5, dev_down, "own"),
                    z=part(rz, 6, dev_z, "own"),
                )
        shift_sem = [[arrival() for _ in range(C)] for _ in range(2)]
        shifts = {}
        for c in range(C):
            shifts[0, c] = message(YS.at[0, c], X.at[1, c, rows(own)], ahead, shift_sent[0], shift_sem[0][c])
            shifts[1, c] = message(YS.at[1, c], SH.at[c], behind, shift_sent[1], shift_sem[1][c])

        def f32(v):
            return v.astype(jnp.float32)

        def project(l, c):
            PB[l, c] = jnp.dot(
                MX[...], O[:, :, c * cw:(c + 1) * cw].reshape(2 * cols, cw), preferred_element_type=jnp.float32
            ).astype(jnp.bfloat16)
            m = rs[l, c]
            for name in ("a0", "a1", "b2") if c % 2 == 0 else ("a0", "a1", "b3"):
                m[name].start()

        def fold_far(l, c):
            m = rs[l, c]
            wait_for(R.at[l, c, pl.ds(0, 2)], rs_sem[c, "far"])
            even = c % 2 == 0
            for slot, b in ((0, up if even else z_up), (1, z_down if even else down)):
                r = rows(b)
                PB[l, c, r] = (f32(PB[l, c, r]) + f32(R[l, c, slot])).astype(jnp.bfloat16)
            m["b3" if even else "b2"].start()

        def give(l, c):
            for name in ("b0", "b1"):
                rs[l, c][name].start()

        def fold_z(l, c):
            m = rs[l, c]
            wait_for(R.at[l, c, pl.ds(2, 2)], rs_sem[c, "z"])
            r = rows(rz)
            PB[l, c, r] = (f32(PB[l, c, r]) + f32(R[l, c, 2]) + f32(R[l, c, 3])).astype(jnp.bfloat16)
            m["z"].start()

        def finish(l, c):
            wait_for(R.at[l, c, pl.ds(4, 3)], rs_sem[c, "own"])
            r = rows(own)
            total = f32(PB[l, c, r]) + f32(R[l, c, 4]) + f32(R[l, c, 5]) + f32(R[l, c, 6])
            result = (f32(X[l, c, r]) + total).astype(jnp.bfloat16)
            YS[l, c] = result
            pltpu.make_async_copy(YS.at[l, c], out.at[l, 0, :, span(c)], out_sem.at[l]).start()

            @pl.when(jnp.logical_not(last) if l == 0 else jnp.logical_not(first))
            def _():
                shifts[l, c].start()

        entered = []

        def enter(c):
            @pl.when(first)
            def _():
                if not entered:
                    wait_for(YS.at[0], fresh_sem_all)

            @pl.when(jnp.logical_not(first))
            def _():
                shifts[0, c].wait_recv()

            entered.append(c)
            spread(1, c)

        def leave(c):
            @pl.when(jnp.logical_not(last))
            def _():
                shifts[1, c].wait_recv()

            pltpu.make_async_copy(SH.at[c], shadow.at[0, :, span(c)], out_sem.at[2]).start()

        def run(steps, order):
            for k, c in order:
                with jax.named_scope(f"step{k}c{c}"):
                    steps[k](c)

        gain_waited = []

        def compute_first(c):
            gathered(0, c)
            if not gain_waited:
                gain_other.wait_recv()
                gain_waited.append(True)
                w_own.wait()
            w_other[c].wait_recv()
            multiply(0, c)

        run({
            4: spread_first,
            5: lambda c: relay_z(0, c),
            6: lambda c: relay_y(0, c),
            7: lambda c: relay_far(0, c),
            8: compute_first,
        }, FIRST_ORDER)
        segments_other.wait_recv()

        @pl.when(jnp.logical_not(last))
        def _():
            segments_ahead.start()

        table_copy.wait()
        with jax.named_scope("attend_first"):
            attend(0)
        o_own.wait()
        o_other.wait_recv()

        def compute_second(c):
            gathered(1, c)
            multiply(1, c)

        run({
            0: lambda c: project(0, c),
            1: lambda c: fold_far(0, c),
            2: lambda c: fold_z(0, c),
            3: lambda c: finish(0, c),
            4: enter,
            5: lambda c: relay_z(1, c),
            6: lambda c: relay_y(1, c),
            7: lambda c: relay_far(1, c),
            8: compute_second,
            9: lambda c: give(0, c),
        }, MIDDLE_ORDER)

        @pl.when(first)
        def _():
            for b in range(2):
                SEGS[1, b] = jnp.broadcast_to(FIN[b:b + 1], (8, half))

        @pl.when(jnp.logical_not(first))
        def _():
            segments_ahead.wait_recv()

        with jax.named_scope("attend_second"):
            attend(1)
        run({
            0: lambda c: project(1, c),
            1: lambda c: fold_far(1, c),
            2: lambda c: fold_z(1, c),
            3: lambda c: finish(1, c),
            4: leave,
            9: lambda c: give(1, c),
        }, LAST_ORDER)
        with jax.named_scope("drain"):
            for l in range(2):
                wait_for(R.at[l], ag_sent[l])
                wait_for(R.at[l], rs_sent[l])
            wait_for(W.at[core], w_sent)
            for ref, n in ((YS.at[0], 0), (YS.at[1], 1), (SH, 2)):
                wait_for(ref, out_sem.at[n])
            for copy in (gain_other, segments_other, o_other):
                copy.wait_send()

        @pl.when(core == 0)
        def _():
            for copy in unsent_early:
                copy.wait_send()

        @pl.when(jnp.logical_not(last))
        def _():
            segments_ahead.wait_send()
            wait_for(YS.at[0], shift_sent[0])

        @pl.when(jnp.logical_not(first))
        def _():
            wait_for(YS.at[1], shift_sent[1])

    bf, f4 = jnp.bfloat16, jnp.float32
    heads = 2 * heads_each
    scratch = [
        pltpu.VMEM((2, C, half, cw), bf),
        pltpu.VMEM((2, 3, width, cols), bf),
        pltpu.VMEM((2, cols, width), bf),
        pltpu.VMEM((2, 3, half, cols), f4),
        pltpu.VMEM((half, HD), f4),
        pltpu.VMEM((half, cw), bf),
        pltpu.VMEM((2, C, half, cw), bf),
        pltpu.VMEM((2, C, 7, block, cw), bf),
        pltpu.VMEM((2, C, block, cw), bf),
        pltpu.VMEM((C, block, cw), bf),
        pltpu.VMEM((2, 2, heads, half, HD), bf),
        pltpu.VMEM((2, 2, heads, half, HD), bf),
        pltpu.VMEM((half, heads * HD), bf),
        pltpu.VMEM((heads, half, half), f4),
        pltpu.VMEM((2, half, half), f4),
        pltpu.VMEM((2, 8, gw), f4),
        pltpu.VMEM((2, 2, 8, half), jnp.int32),
        pltpu.VMEM((2, half, HD), f4),
        pltpu.VMEM((1, gw), bf),
        pltpu.VMEM((1, half), jnp.int32),
        pltpu.VMEM((2, half), jnp.int32),
        pltpu.SemaphoreType.DMA((C + 7,)),
        pltpu.SemaphoreType.DMA((6 + 1 + 4 + 4,)),
        pltpu.SemaphoreType.DMA(((4 + 3 + 2 + 1) * C + 4 + 4,)),
        pltpu.SemaphoreType.DMA((3,)),
    ]
    return kernel, scratch


def store(count):
    def kernel(*refs):
        sources, results, held, sem = refs[:count], refs[count:2 * count], refs[2 * count:3 * count], refs[-1]
        for i in range(count):
            pltpu.make_async_copy(sources[i], held[i], sem.at[0, i]).start()
        for i in range(count):
            pltpu.make_async_copy(sources[i], held[i], sem.at[0, i]).wait()
            pltpu.make_async_copy(held[i], results[i], sem.at[1, i]).start()
        for i in range(count):
            pltpu.make_async_copy(held[i], results[i], sem.at[1, i]).wait()

    return kernel


def carry_over(arrays):
    hbm = pl.BlockSpec(memory_space=pl.ANY)
    return pl.pallas_call(
        store(len(arrays)),
        name="store",
        out_shape=tuple(jax.ShapeDtypeStruct(a.shape, a.dtype) for a in arrays),
        in_specs=[hbm] * len(arrays),
        out_specs=(hbm,) * len(arrays),
        scratch_shapes=[pltpu.VMEM(a.shape, a.dtype) for a in arrays] + [pltpu.SemaphoreType.DMA((2, len(arrays)))],
        compiler_params=pltpu.CompilerParams(vmem_limit_bytes=60 * 2**20),
    )(*arrays)


def per_device(carried, carried_segments, fresh_batch, fresh_segments, qkv_weight, out_weight, norm_gain):
    _, block, width = carried.shape
    cols = qkv_weight.shape[-1]
    n_sections = lax.axis_size("section") // 2
    kernel, scratch = make_kernel(n_sections, width, block, cols // HD)
    weights = jnp.transpose(qkv_weight[0], (1, 0, 2))
    tables = jnp.asarray(rope_tables(16 * block))
    hbm = pl.BlockSpec(memory_space=pltpu.HBM)
    out, shadow = pl.pallas_call(
        kernel,
        name="relay",
        out_shape=(
            jax.ShapeDtypeStruct((2, 1, block, width), jnp.bfloat16),
            jax.ShapeDtypeStruct((1, block, width), jnp.bfloat16),
        ),
        in_specs=[hbm] * 8,
        out_specs=(hbm, hbm),
        scratch_shapes=scratch,
        compiler_params=pltpu.CompilerParams(
            collective_id=0, has_side_effects=True, vmem_limit_bytes=60 * 2**20
        ),
    )(carried, carried_segments, fresh_batch, fresh_segments, weights, out_weight, norm_gain, tables)
    return carry_over((out, shadow))


def solution(mesh):
    return jax.shard_map(
        per_device,
        mesh=mesh,
        in_specs=(
            P("section", "tp", None),
            P("section", None),
            P(None, "tp", None),
            P(),
            P("section", None, None, "tp"),
            P("section", "tp", None),
            P("section", None),
        ),
        out_specs=(P(None, "section", "tp", None), P("section", "tp", None)),
        check_vma=False,
    )
```

```python
import jax
import jax.numpy as jnp
import numpy as np
from jax import lax
from jax.experimental import pallas as pl
from jax.experimental.pallas import tpu as pltpu
from jax.sharding import PartitionSpec as P

HD = 128
EPS = 1e-05
ROPE_BASE = 10000.0
MASKED = -1e30
MESH = pl.DeviceIdType.MESH
CHUNKS = 10
FIRST_ORDER = (
    (4, 6), (4, 1), (4, 7), (4, 9), (4, 4), (4, 5), (6, 1), (4, 8), (4, 3), (6, 7),
    (4, 2), (6, 9), (4, 0), (6, 6), (5, 5), (6, 4), (6, 8), (7, 1), (6, 0), (6, 2),
    (5, 6), (6, 5), (6, 3), (7, 7), (5, 4), (5, 9), (7, 6), (7, 9), (5, 7), (7, 4),
    (5, 0), (7, 8), (7, 5), (5, 8), (7, 0), (5, 1), (5, 3), (8, 6), (7, 2), (8, 4),
    (7, 3), (5, 2), (8, 9), (8, 7), (8, 5), (8, 0), (8, 8), (8, 1), (8, 3), (8, 2),
)
MIDDLE_ORDER = (
    (0, 5), (0, 7), (0, 6), (0, 4), (0, 3), (0, 9), (10, 5), (0, 8), (0, 2), (2, 6),
    (2, 4), (2, 5), (0, 1), (1, 9), (0, 0), (2, 7), (10, 2), (2, 3), (1, 5), (10, 3),
    (9, 5), (10, 4), (1, 8), (2, 2), (2, 9), (9, 9), (2, 0), (10, 0), (2, 1), (10, 1),
    (1, 3), (10, 6), (1, 2), (9, 2), (3, 5), (2, 8), (3, 9), (9, 8), (10, 7), (3, 2),
    (1, 6), (9, 3), (1, 4), (1, 1), (9, 4), (4, 5), (3, 8), (1, 7), (9, 6), (3, 3),
    (9, 1), (9, 7), (3, 4), (1, 0), (4, 2), (5, 5), (4, 8), (3, 7), (3, 6), (9, 0),
    (4, 9), (4, 4), (6, 5), (5, 8), (6, 8), (6, 9), (3, 1), (6, 2), (3, 0), (4, 7),
    (6, 4), (5, 2), (7, 5), (4, 6), (4, 3), (5, 9), (7, 9), (4, 1), (7, 2), (4, 0),
    (6, 7), (6, 6), (6, 3), (6, 1), (7, 4), (5, 3), (5, 6), (7, 8), (6, 0), (5, 4),
    (8, 9), (7, 6), (7, 7), (8, 2), (5, 7), (7, 1), (5, 1), (5, 0), (7, 3), (8, 5),
    (7, 0), (8, 8), (8, 6), (8, 4), (8, 7), (8, 1), (8, 3), (8, 0),
)
LAST_ORDER = (
    (0, 8), (0, 5), (0, 6), (0, 0), (0, 4), (0, 2), (10, 5), (1, 8), (0, 3), (0, 1),
    (2, 5), (0, 7), (2, 6), (10, 6), (2, 2), (1, 5), (9, 5), (10, 4), (10, 0), (10, 1),
    (2, 0), (2, 4), (2, 8), (9, 8), (10, 7), (2, 1), (10, 2), (1, 6), (2, 7), (9, 6),
    (0, 9), (3, 5), (1, 1), (2, 3), (9, 1), (3, 8), (10, 3), (1, 2), (9, 2), (1, 4),
    (3, 6), (1, 0), (9, 0), (9, 4), (1, 7), (3, 1), (1, 3), (1, 9), (3, 2), (9, 7),
    (3, 4), (9, 3), (2, 9), (3, 0), (4, 1), (4, 6), (3, 3), (9, 9), (3, 7), (4, 2),
    (3, 9), (4, 8), (4, 4), (4, 3), (4, 7), (4, 5), (4, 0), (4, 9),
)
ALONG_Z = ((0, 1, 2, 3, 4, 5, 6, 7), (0, 1, 2, 3, 4, 5, 6, 7))


def rope_tables(tokens):
    frequency = np.float32(ROPE_BASE) ** (-(np.arange(HD // 2, dtype=np.float32) * np.float32(2.0) / np.float32(HD)))
    angles = np.arange(tokens, dtype=np.float32)[:, None] * frequency.astype(np.float32)[None, :]
    cosine = np.cos(angles.astype(np.float64)).astype(np.float32)
    sine = np.sin(angles.astype(np.float64)).astype(np.float32)
    cosines = np.concatenate([cosine, cosine], axis=1)
    sines = np.concatenate([-sine, sine], axis=1)
    return np.stack([cosines, sines], axis=0)


def make_kernel(n_sections, width, block, heads_each):
    C = CHUNKS
    half = 8 * block
    cw = width // C
    gw = width // 2
    cols = heads_each * HD

    def kernel(
        carried, own_segments, fresh, fresh_segments, w_hbm, o_hbm, gain, tables,
        out, shadow,
        X, W, O, ACC, SS, XG, PB, R, YS, SH, KV, KVO, MX, S, BIAS, G, SEGS, TAB, GIN, SIN, FIN,
        local_sem, send_sem, recv_sem, out_sem,
    ):
        p = lax.axis_index("section")
        t = lax.axis_index("tp")
        core = lax.rem(p, 2)
        s = lax.div(p, 2)
        zl = lax.div(t, 4)
        y = lax.rem(t, 4)
        first = s == 0
        last = s == n_sections - 1

        def at(z, yy):
            return z * 4 + lax.rem(yy, 4)

        other_z = 1 - zl
        own, rz = t, at(other_z, y)
        up, down, far = at(zl, y + 1), at(zl, y + 3), at(zl, y + 2)
        z_up, z_down, z_far = at(other_z, y + 1), at(other_z, y + 3), at(other_z, y + 2)
        dev_z, dev_up, dev_down = (p, rz), (p, up), (p, down)
        partner = (p + 1 - 2 * core, t)
        ahead = (lax.rem(p + 2, 2 * n_sections), t)
        behind = (lax.rem(p + 2 * n_sections - 2, 2 * n_sections), t)

        def rows(b):
            return pl.ds(pl.multiple_of(b * block, block), block)

        def span(c):
            return pl.ds(c * cw, cw)

        counts = {"local": 0, "sent": 0, "received": 0}

        def fresh_sem(kind, sems):
            n = counts[kind]
            counts[kind] += 1
            return sems.at[n]

        def local_copy(src, dst):
            return pltpu.make_async_copy(src, dst, fresh_sem("local", local_sem))

        unsent_early = []

        def send_group():
            return fresh_sem("sent", send_sem)

        def arrival():
            return fresh_sem("received", recv_sem)

        def message(src, dst, device, sent, arrived):
            return pltpu.make_async_remote_copy(
                src_ref=src, dst_ref=dst, send_sem=sent, recv_sem=arrived,
                device_id=device, device_id_type=MESH,
            )

        def wait_for(ref, sem):
            pltpu.make_async_copy(ref, ref, sem).wait()

        small_loads = [local_copy(gain, GIN), local_copy(own_segments, SIN), local_copy(fresh_segments, FIN)]
        for copy in small_loads:
            copy.start()
        own_rows = []
        for c in range(C):
            copy = local_copy(carried.at[0, :, span(c)], X.at[0, c, rows(own)])
            copy.start()
            own_rows.append(copy)
        w_own = local_copy(w_hbm, W.at[core])
        w_own.start()
        o_own = local_copy(o_hbm.at[0], O.at[core])
        o_own.start()
        table_copy = local_copy(tables.at[:, pl.ds(pl.multiple_of(core * half, half), half)], TAB)
        table_copy.start()
        fresh_sem_all = fresh_sem("local", local_sem)
        fresh_rows = [
            pltpu.make_async_copy(fresh.at[core, :, span(c)], X.at[1, c, rows(own)], fresh_sem_all) for c in range(C)
        ]

        @pl.when(last)
        def _():
            SH[...] = jnp.zeros(SH.shape, SH.dtype)

        @pl.when(first)
        def _():
            for copy in fresh_rows:
                copy.start()

        barrier = pltpu.get_barrier_semaphore()
        for device in (dev_z, dev_up, dev_down, partner, ahead, behind):
            pl.semaphore_signal(barrier, inc=1, device_id=device, device_id_type=MESH)
        with jax.named_scope("entry"):
            pl.semaphore_wait(barrier, 6)
        for copy in small_loads:
            copy.wait()
        G[core] = jnp.broadcast_to(GIN[...].astype(jnp.float32), (8, gw))
        SEGS[0, core] = jnp.broadcast_to(SIN[...], (8, half))

        ag_sent = [send_group() for _ in range(2)]
        rs_sent = [send_group() for _ in range(2)]
        shift_sent = [send_group() for _ in range(2)]
        ag_sem = {(c, k): arrival() for c in range(C) for k in ("z", "y", "far", "rest")}
        rs_sem = {(c, k): arrival() for c in range(C) for k in ("q", "a", "z", "own")}

        ag = {}
        for l in range(2):
            for c in range(C):
                def block_of(b, device, kind, l=l, c=c):
                    ref = X.at[l, c, rows(b)]
                    return message(ref, ref, device, ag_sent[l], ag_sem[c, kind])
                even = c % 2 == 0
                ag[l, c] = dict(
                    z=block_of(own, dev_z, "z"),
                    down=block_of(own, dev_up, "y" if even else "rest"),
                    up=block_of(own, dev_down, "rest" if even else "y"),
                    z_down=block_of(rz, dev_up, "rest"),
                    z_up=block_of(rz, dev_down, "rest"),
                    far=block_of(down, dev_up, "far") if even else block_of(up, dev_down, "far"),
                    z_far=block_of(far, dev_z, "rest"),
                )

        def spread(l, c):
            for name in ("z", "down", "up"):
                ag[l, c][name].start()

        def relay_z(l, c):
            wait_for(X.at[l, c, rows(rz)], ag_sem[c, "z"])
            ag[l, c]["z_down"].start()
            ag[l, c]["z_up"].start()

        def relay_y(l, c):
            wait_for(X.at[l, c, rows(down if c % 2 == 0 else up)], ag_sem[c, "y"])
            ag[l, c]["far"].start()

        def relay_far(l, c):
            wait_for(X.at[l, c, rows(far)], ag_sem[c, "far"])
            ag[l, c]["z_far"].start()

        def gathered(l, c):
            wait_for(X.at[l, c, pl.ds(0, 4 * block)], ag_sem[c, "rest"])

        def spread_first(c):
            own_rows[c].wait()
            spread(0, c)

        w_sent = send_group()
        w_sem = [arrival() for _ in range(C)]
        small_sent, small_sem = [send_group() for _ in range(4)], [arrival() for _ in range(4)]
        w_other = {}
        for c in (c for k, c in FIRST_ORDER if k == 8):
            w_other[c] = message(w_hbm.at[:, span(c)], W.at[core, :, span(c)], partner, w_sent, w_sem[c])
            w_other[c].start()
            if len(w_other) == 1:
                gain_other = message(G.at[core], G.at[core], partner, small_sent[0], small_sem[0])
                gain_other.start()
                segments_other = message(
                    SEGS.at[0, core], SEGS.at[0, core], partner, small_sent[1], small_sem[1]
                )
                segments_other.start()
        o_other = message(o_hbm.at[0], O.at[core], partner, small_sent[2], small_sem[2])
        o_other.start()
        segments_ahead = message(SEGS.at[0], SEGS.at[1], ahead, small_sent[3], small_sem[3])

        begun = set()

        def multiply(l, c):
            opening = l not in begun
            begun.add(l)
            g0 = (c * cw) // gw
            scale = G[g0, 0:1, (c * cw) % gw:(c * cw) % gw + cw]

            def body(i, _):
                r = pl.ds(pl.multiple_of(i * 32, 32), 32)
                x = X[l, c, r].astype(jnp.float32)
                XG[r] = (x * scale).astype(jnp.bfloat16)
                square = x * x
                total = square[:, 0:HD]
                for k in range(1, cw // HD):
                    total = total + square[:, k * HD:(k + 1) * HD]
                if opening:
                    SS[r] = total
                else:
                    SS[r] = SS[r] + total
                return 0

            lax.fori_loop(0, half // 32, body, 0)
            for g in range(2):
                for j in range(3):
                    part = jnp.dot(XG[...], W[g, j, c * cw:(c + 1) * cw], preferred_element_type=jnp.float32)
                    if opening:
                        ACC[g, j] = part
                    else:
                        ACC[g, j] = ACC[g, j] + part

        def prepare(l):
            mine = jnp.broadcast_to(SEGS[l, core, 0:1], (HD, half)).astype(jnp.float32).T[:, 0:1]
            row_of = lax.broadcasted_iota(jnp.int32, (half, half), 0)
            column_of = lax.broadcasted_iota(jnp.int32, (half, half), 1)
            same = mine == SEGS[l, core, 0:1].astype(jnp.float32)
            BIAS[0] = jnp.where(same & (column_of <= row_of), 0.0, MASKED)
            BIAS[1] = jnp.where(mine == SEGS[l, 0, 0:1].astype(jnp.float32), 0.0, MASKED)

        def attend(l):
            power = jnp.sum(SS[...], axis=-1, keepdims=True) * (1.0 / width)
            factor = lax.rsqrt(power + EPS)
            heads = [(g, i) for g in range(2) for i in range(heads_each)]

            def rotated(v):
                return v * TAB[0] + pltpu.roll(v, HD // 2, 1) * TAB[1]

            for h, (g, i) in enumerate(heads):
                KV[l, 1, h] = (ACC[g, 2, :, i * HD:(i + 1) * HD] * factor).astype(jnp.bfloat16)
            values = message(KV.at[l, 1], KVO.at[l, 1], partner, send_group(), arrival())
            keys = message(KV.at[l, 0], KVO.at[l, 0], partner, send_group(), arrival())

            @pl.when(core == 0)
            def _():
                values.start()

            for h, (g, i) in enumerate(heads):
                KV[l, 0, h] = rotated(ACC[g, 1, :, i * HD:(i + 1) * HD] * factor).astype(jnp.bfloat16)

            @pl.when(core == 0)
            def _():
                keys.start()

            unsent_early.append(values)
            unsent_early.append(keys)
            for h, (g, i) in enumerate(heads):
                q = rotated(ACC[g, 0, :, i * HD:(i + 1) * HD] * factor).astype(jnp.bfloat16)
                MX[:, h * HD:(h + 1) * HD] = q
                scores = lax.dot_general(q, KV[l, 0, h], (((1,), (1,)), ((), ())), preferred_element_type=jnp.float32)
                near = scores * HD ** (-0.5) + BIAS[0]
                top = jnp.max(near, axis=-1, keepdims=True)
                near = jnp.exp(near - top)
                total = jnp.sum(near, axis=-1, keepdims=True)
                S[h, :, 0:HD] = jnp.broadcast_to(top, (half, HD))
                S[h, :, HD:2 * HD] = jnp.broadcast_to(total, (half, HD))
                S[h, :, 2 * HD:] = jnp.dot(near.astype(jnp.bfloat16), KV[l, 1, h], preferred_element_type=jnp.float32)

            def columns(h):
                return slice(h * HD, (h + 1) * HD)

            @pl.when(core == 0)
            def _():
                for h in range(len(heads)):
                    MX[:, columns(h)] = (S[h, :, 2 * HD:] / S[h, :, HD:2 * HD]).astype(jnp.bfloat16)

            @pl.when(core == 1)
            def _():
                with jax.named_scope("keys_wait"):
                    values.wait_recv()
                    keys.wait_recv()
                for h in range(len(heads)):
                    away = lax.dot_general(
                        MX[:, columns(h)], KVO[l, 0, h], (((1,), (1,)), ((), ())), preferred_element_type=jnp.float32
                    )
                    away = away * HD ** (-0.5) + BIAS[1]
                    before = S[h, :, 0:HD]
                    top = jnp.maximum(before, jnp.max(away, axis=-1, keepdims=True))
                    kept = jnp.exp(before - top)
                    away = jnp.exp(away - top[:, 0:1])
                    total = S[h, :, HD:2 * HD] * kept + jnp.sum(away, axis=-1, keepdims=True)
                    mixed = S[h, :, 2 * HD:] * kept
                    mixed = mixed + jnp.dot(away.astype(jnp.bfloat16), KVO[l, 1, h], preferred_element_type=jnp.float32)
                    MX[:, columns(h)] = (mixed / total).astype(jnp.bfloat16)

        rs = {}
        for l in range(2):
            for c in range(C):
                def part(b, slot, device, kind, l=l, c=c):
                    return message(PB.at[l, c, rows(b)], R.at[l, c, slot], device, rs_sent[l], rs_sem[c, kind])
                even = c % 2 == 0
                rs[l, c] = dict(
                    b2=part(z_up, 2, dev_up, "z"),
                    b3=part(z_down, 3, dev_down, "z"),
                    b0=part(up, 4, dev_up, "own"),
                    b1=part(down, 5, dev_down, "own"),
                    z=part(rz, 6, dev_z, "own"),
                )
                if c in ALONG_Z[l]:
                    rs[l, c].update(q=part(z_far, 0, dev_z, "q"), a=part(far, 1, dev_up if even else dev_down, "a"))
                else:
                    rs[l, c].update(
                        a0=part(far if even else z_far, 0, dev_up, "q"), a1=part(z_far if even else far, 1, dev_down, "a")
                    )
        shift_sem = [[arrival() for _ in range(C)] for _ in range(2)]
        shifts = {}
        for c in range(C):
            shifts[0, c] = message(YS.at[0, c], X.at[1, c, rows(own)], ahead, shift_sent[0], shift_sem[0][c])
            shifts[1, c] = message(YS.at[1, c], SH.at[c], behind, shift_sent[1], shift_sem[1][c])

        def f32(v):
            return v.astype(jnp.float32)

        def project(l, c):
            PB[l, c] = jnp.dot(
                MX[...], O[:, :, c * cw:(c + 1) * cw].reshape(2 * cols, cw), preferred_element_type=jnp.float32
            ).astype(jnp.bfloat16)
            m = rs[l, c]
            for name in ("q", "b2", "b3") if c in ALONG_Z[l] else ("a0", "a1", "b2" if c % 2 == 0 else "b3"):
                m[name].start()

        def fold(l, c, slot, kind, b):
            wait_for(R.at[l, c, slot], rs_sem[c, kind])
            r = rows(b)
            PB[l, c, r] = (f32(PB[l, c, r]) + f32(R[l, c, slot])).astype(jnp.bfloat16)

        def fold_far(l, c):
            fold(l, c, 0, "q", far)
            rs[l, c]["a"].start()

        def fold_y(l, c):
            even = c % 2 == 0
            if c in ALONG_Z[l]:
                fold(l, c, 1, "a", up if even else down)
                return
            fold(l, c, 0, "q", up if even else z_up)
            fold(l, c, 1, "a", z_down if even else down)
            rs[l, c]["b3" if even else "b2"].start()

        def give(l, c):
            for name in ("b0", "b1"):
                rs[l, c][name].start()

        def fold_z(l, c):
            m = rs[l, c]
            wait_for(R.at[l, c, pl.ds(2, 2)], rs_sem[c, "z"])
            r = rows(rz)
            PB[l, c, r] = (f32(PB[l, c, r]) + f32(R[l, c, 2]) + f32(R[l, c, 3])).astype(jnp.bfloat16)
            m["z"].start()

        def finish(l, c):
            wait_for(R.at[l, c, pl.ds(4, 3)], rs_sem[c, "own"])
            r = rows(own)
            total = f32(PB[l, c, r]) + f32(R[l, c, 4]) + f32(R[l, c, 5]) + f32(R[l, c, 6])
            result = (f32(X[l, c, r]) + total).astype(jnp.bfloat16)
            YS[l, c] = result
            pltpu.make_async_copy(YS.at[l, c], out.at[l, 0, :, span(c)], out_sem.at[l]).start()

            @pl.when(jnp.logical_not(last) if l == 0 else jnp.logical_not(first))
            def _():
                shifts[l, c].start()

        entered = []

        def enter(c):
            @pl.when(first)
            def _():
                if not entered:
                    wait_for(YS.at[0], fresh_sem_all)

            @pl.when(jnp.logical_not(first))
            def _():
                shifts[0, c].wait_recv()

            entered.append(c)
            spread(1, c)

        def leave(c):
            @pl.when(jnp.logical_not(last))
            def _():
                shifts[1, c].wait_recv()

            pltpu.make_async_copy(SH.at[c], shadow.at[0, :, span(c)], out_sem.at[2]).start()

        def run(steps, order):
            for k, c in order:
                with jax.named_scope(f"step{k}c{c}"):
                    steps[k](c)

        gain_waited = []

        def compute_first(c):
            gathered(0, c)
            if not gain_waited:
                gain_other.wait_recv()
                gain_waited.append(True)
                w_own.wait()
                segments_other.wait_recv()

                @pl.when(jnp.logical_not(last))
                def _():
                    segments_ahead.start()

                prepare(0)
            w_other[c].wait_recv()
            multiply(0, c)

        run({
            4: spread_first,
            5: lambda c: relay_z(0, c),
            6: lambda c: relay_y(0, c),
            7: lambda c: relay_far(0, c),
            8: compute_first,
        }, FIRST_ORDER)
        table_copy.wait()
        with jax.named_scope("attend_first"):
            attend(0)
        o_own.wait()
        o_other.wait_recv()

        def segments_second():
            @pl.when(first)
            def _():
                for b in range(2):
                    SEGS[1, b] = jnp.broadcast_to(FIN[b:b + 1], (8, half))

            @pl.when(jnp.logical_not(first))
            def _():
                segments_ahead.wait_recv()
            prepare(1)

        def compute_second(c):
            if 1 not in begun:
                segments_second()
            gathered(1, c)
            multiply(1, c)

        run({
            0: lambda c: project(0, c),
            1: lambda c: fold_y(0, c),
            10: lambda c: fold_far(0, c),
            2: lambda c: fold_z(0, c),
            3: lambda c: finish(0, c),
            4: enter,
            5: lambda c: relay_z(1, c),
            6: lambda c: relay_y(1, c),
            7: lambda c: relay_far(1, c),
            8: compute_second,
            9: lambda c: give(0, c),
        }, MIDDLE_ORDER)

        with jax.named_scope("attend_second"):
            attend(1)
        run({
            0: lambda c: project(1, c),
            1: lambda c: fold_y(1, c),
            10: lambda c: fold_far(1, c),
            2: lambda c: fold_z(1, c),
            3: lambda c: finish(1, c),
            4: leave,
            9: lambda c: give(1, c),
        }, LAST_ORDER)
        with jax.named_scope("drain"):
            for l in range(2):
                wait_for(R.at[l], ag_sent[l])
                wait_for(R.at[l], rs_sent[l])
            wait_for(W.at[core], w_sent)
            for ref, n in ((YS.at[0], 0), (YS.at[1], 1), (SH, 2)):
                wait_for(ref, out_sem.at[n])
            for copy in (gain_other, segments_other, o_other):
                copy.wait_send()

        @pl.when(core == 0)
        def _():
            for copy in unsent_early:
                copy.wait_send()

        @pl.when(jnp.logical_not(last))
        def _():
            segments_ahead.wait_send()
            wait_for(YS.at[0], shift_sent[0])

        @pl.when(jnp.logical_not(first))
        def _():
            wait_for(YS.at[1], shift_sent[1])

    bf, f4 = jnp.bfloat16, jnp.float32
    heads = 2 * heads_each
    scratch = [
        pltpu.VMEM((2, C, half, cw), bf),
        pltpu.VMEM((2, 3, width, cols), bf),
        pltpu.VMEM((2, cols, width), bf),
        pltpu.VMEM((2, 3, half, cols), f4),
        pltpu.VMEM((half, HD), f4),
        pltpu.VMEM((half, cw), bf),
        pltpu.VMEM((2, C, half, cw), bf),
        pltpu.VMEM((2, C, 7, block, cw), bf),
        pltpu.VMEM((2, C, block, cw), bf),
        pltpu.VMEM((C, block, cw), bf),
        pltpu.VMEM((2, 2, heads, half, HD), bf),
        pltpu.VMEM((2, 2, heads, half, HD), bf),
        pltpu.VMEM((half, heads * HD), bf),
        pltpu.VMEM((heads, half, 3 * HD), f4),
        pltpu.VMEM((2, half, half), f4),
        pltpu.VMEM((2, 8, gw), f4),
        pltpu.VMEM((2, 2, 8, half), jnp.int32),
        pltpu.VMEM((2, half, HD), f4),
        pltpu.VMEM((1, gw), bf),
        pltpu.VMEM((1, half), jnp.int32),
        pltpu.VMEM((2, half), jnp.int32),
        pltpu.SemaphoreType.DMA((C + 7,)),
        pltpu.SemaphoreType.DMA((6 + 1 + 4 + 4,)),
        pltpu.SemaphoreType.DMA(((4 + 4 + 2 + 1) * C + 4 + 4,)),
        pltpu.SemaphoreType.DMA((3,)),
    ]
    return kernel, scratch


def store(count):
    def kernel(*refs):
        sources, results, held, sem = refs[:count], refs[count:2 * count], refs[2 * count:3 * count], refs[-1]
        for i in range(count):
            pltpu.make_async_copy(sources[i], held[i], sem.at[0, i]).start()
        for i in range(count):
            pltpu.make_async_copy(sources[i], held[i], sem.at[0, i]).wait()
            pltpu.make_async_copy(held[i], results[i], sem.at[1, i]).start()
        for i in range(count):
            pltpu.make_async_copy(held[i], results[i], sem.at[1, i]).wait()

    return kernel


def carry_over(arrays):
    hbm = pl.BlockSpec(memory_space=pl.ANY)
    return pl.pallas_call(
        store(len(arrays)),
        name="store",
        out_shape=tuple(jax.ShapeDtypeStruct(a.shape, a.dtype) for a in arrays),
        in_specs=[hbm] * len(arrays),
        out_specs=(hbm,) * len(arrays),
        scratch_shapes=[pltpu.VMEM(a.shape, a.dtype) for a in arrays] + [pltpu.SemaphoreType.DMA((2, len(arrays)))],
        compiler_params=pltpu.CompilerParams(vmem_limit_bytes=60 * 2**20),
    )(*arrays)


def per_device(carried, carried_segments, fresh_batch, fresh_segments, qkv_weight, out_weight, norm_gain):
    _, block, width = carried.shape
    cols = qkv_weight.shape[-1]
    n_sections = lax.axis_size("section") // 2
    kernel, scratch = make_kernel(n_sections, width, block, cols // HD)
    weights = jnp.transpose(qkv_weight[0], (1, 0, 2))
    tables = jnp.asarray(rope_tables(16 * block))
    hbm = pl.BlockSpec(memory_space=pltpu.HBM)
    out, shadow = pl.pallas_call(
        kernel,
        name="relay",
        out_shape=(
            jax.ShapeDtypeStruct((2, 1, block, width), jnp.bfloat16),
            jax.ShapeDtypeStruct((1, block, width), jnp.bfloat16),
        ),
        in_specs=[hbm] * 8,
        out_specs=(hbm, hbm),
        scratch_shapes=scratch,
        compiler_params=pltpu.CompilerParams(
            collective_id=0, has_side_effects=True, vmem_limit_bytes=60 * 2**20
        ),
    )(carried, carried_segments, fresh_batch, fresh_segments, weights, out_weight, norm_gain, tables)
    return carry_over((out, shadow))


def solution(mesh):
    return jax.shard_map(
        per_device,
        mesh=mesh,
        in_specs=(
            P("section", "tp", None),
            P("section", None),
            P(None, "tp", None),
            P(),
            P("section", None, None, "tp"),
            P("section", "tp", None),
            P("section", None),
        ),
        out_specs=(P(None, "section", "tp", None), P("section", "tp", None)),
        check_vma=False,
    )
```

```python
import jax
import jax.numpy as jnp
import numpy as np
from jax import lax
from jax.experimental import pallas as pl
from jax.experimental.pallas import tpu as pltpu
from jax.sharding import PartitionSpec as P

HD = 128
EPS = 1e-05
ROPE_BASE = 10000.0
MASKED = -1e30
MESH = pl.DeviceIdType.MESH
CHUNKS = 10
FIRST_ORDER = (
    (4, 6), (4, 1), (4, 7), (4, 9), (4, 4), (4, 5), (6, 1), (4, 8), (4, 3), (6, 7),
    (4, 2), (6, 9), (4, 0), (6, 6), (5, 5), (6, 4), (6, 8), (7, 1), (6, 0), (6, 2),
    (5, 6), (6, 5), (6, 3), (7, 7), (5, 4), (5, 9), (7, 6), (7, 9), (5, 7), (7, 4),
    (5, 0), (7, 8), (7, 5), (5, 8), (7, 0), (5, 1), (5, 3), (8, 6), (7, 2), (8, 4),
    (7, 3), (5, 2), (8, 9), (8, 7), (8, 5), (8, 0), (8, 8), (8, 1), (8, 3), (8, 2),
)
MIDDLE_ORDER = (
    (0, 5), (0, 7), (0, 6), (0, 4), (0, 3), (0, 9), (10, 5), (0, 8), (0, 2), (2, 6),
    (2, 4), (2, 5), (0, 1), (1, 9), (0, 0), (2, 7), (10, 2), (2, 3), (1, 5), (10, 3),
    (9, 5), (10, 4), (1, 8), (2, 2), (2, 9), (9, 9), (2, 0), (10, 0), (2, 1), (10, 1),
    (1, 3), (10, 6), (1, 2), (9, 2), (3, 5), (2, 8), (3, 9), (9, 8), (10, 7), (3, 2),
    (1, 6), (9, 3), (1, 4), (1, 1), (9, 4), (4, 5), (3, 8), (1, 7), (9, 6), (3, 3),
    (9, 1), (9, 7), (3, 4), (1, 0), (4, 2), (5, 5), (4, 8), (3, 7), (3, 6), (9, 0),
    (4, 9), (4, 4), (6, 5), (5, 8), (6, 8), (6, 9), (3, 1), (6, 2), (3, 0), (4, 7),
    (6, 4), (5, 2), (7, 5), (4, 6), (4, 3), (5, 9), (7, 9), (4, 1), (7, 2), (4, 0),
    (6, 7), (6, 6), (6, 3), (6, 1), (7, 4), (5, 3), (5, 6), (7, 8), (6, 0), (5, 4),
    (8, 9), (7, 6), (7, 7), (8, 2), (5, 7), (7, 1), (5, 1), (5, 0), (7, 3), (8, 5),
    (7, 0), (8, 8), (8, 6), (8, 4), (8, 7), (8, 1), (8, 3), (8, 0),
)
LAST_ORDER = (
    (0, 8), (0, 5), (0, 6), (0, 0), (0, 4), (0, 2), (10, 5), (1, 8), (0, 3), (0, 1),
    (2, 5), (0, 7), (2, 6), (10, 6), (2, 2), (1, 5), (9, 5), (10, 4), (10, 0), (10, 1),
    (2, 0), (2, 4), (2, 8), (9, 8), (10, 7), (2, 1), (10, 2), (1, 6), (2, 7), (9, 6),
    (0, 9), (3, 5), (1, 1), (2, 3), (9, 1), (3, 8), (10, 3), (1, 2), (9, 2), (1, 4),
    (3, 6), (1, 0), (9, 0), (9, 4), (1, 7), (3, 1), (1, 3), (1, 9), (3, 2), (9, 7),
    (3, 4), (9, 3), (2, 9), (3, 0), (4, 1), (4, 6), (3, 3), (9, 9), (3, 7), (4, 2),
    (3, 9), (4, 8), (4, 4), (4, 3), (4, 7), (4, 5), (4, 0), (4, 9),
)
ALONG_Z = ((0, 1, 2, 3, 4, 5, 6, 7), (0, 1, 2, 3, 4, 5, 6, 7))


def rope_tables(tokens):
    frequency = np.float32(ROPE_BASE) ** (-(np.arange(HD // 2, dtype=np.float32) * np.float32(2.0) / np.float32(HD)))
    angles = np.arange(tokens, dtype=np.float32)[:, None] * frequency.astype(np.float32)[None, :]
    cosine = np.cos(angles.astype(np.float64)).astype(np.float32)
    sine = np.sin(angles.astype(np.float64)).astype(np.float32)
    cosines = np.concatenate([cosine, cosine], axis=1)
    sines = np.concatenate([-sine, sine], axis=1)
    return np.stack([cosines, sines], axis=0)


def make_kernel(n_sections, width, block, heads_each):
    C = CHUNKS
    half = 8 * block
    cw = width // C
    gw = width // 2
    cols = heads_each * HD

    def kernel(
        carried, own_segments, fresh, fresh_segments, w_hbm, o_hbm, gain, tables,
        out, shadow,
        X, W, O, ACC, SS, XG, PB, R, YS, SH, KV, KVO, MX, S, BIAS, G, SEGS, TAB, GIN, SIN, FIN,
        local_sem, send_sem, recv_sem,
    ):
        p = lax.axis_index("section")
        t = lax.axis_index("tp")
        core = lax.rem(p, 2)
        s = lax.div(p, 2)
        zl = lax.div(t, 4)
        y = lax.rem(t, 4)
        first = s == 0
        last = s == n_sections - 1

        def at(z, yy):
            return z * 4 + lax.rem(yy, 4)

        other_z = 1 - zl
        own, rz = t, at(other_z, y)
        up, down, far = at(zl, y + 1), at(zl, y + 3), at(zl, y + 2)
        z_up, z_down, z_far = at(other_z, y + 1), at(other_z, y + 3), at(other_z, y + 2)
        dev_z, dev_up, dev_down = (p, rz), (p, up), (p, down)
        partner = (p + 1 - 2 * core, t)
        ahead = (lax.rem(p + 2, 2 * n_sections), t)
        behind = (lax.rem(p + 2 * n_sections - 2, 2 * n_sections), t)

        def rows(b):
            return pl.ds(pl.multiple_of(b * block, block), block)

        def span(c):
            return pl.ds(c * cw, cw)

        counts = {"local": 0, "sent": 0, "received": 0}

        def fresh_sem(kind, sems):
            n = counts[kind]
            counts[kind] += 1
            return sems.at[n]

        def local_copy(src, dst):
            return pltpu.make_async_copy(src, dst, fresh_sem("local", local_sem))

        unsent_early = []

        def send_group():
            return fresh_sem("sent", send_sem)

        def arrival():
            return fresh_sem("received", recv_sem)

        def message(src, dst, device, sent, arrived):
            return pltpu.make_async_remote_copy(
                src_ref=src, dst_ref=dst, send_sem=sent, recv_sem=arrived,
                device_id=device, device_id_type=MESH,
            )

        def wait_for(ref, sem):
            pltpu.make_async_copy(ref, ref, sem).wait()

        small_loads = [local_copy(gain, GIN), local_copy(own_segments, SIN), local_copy(fresh_segments, FIN)]
        for copy in small_loads:
            copy.start()
        own_rows = []
        for c in range(C):
            copy = local_copy(carried.at[0, :, span(c)], X.at[0, c, rows(own)])
            copy.start()
            own_rows.append(copy)
        w_own = local_copy(w_hbm, W.at[core])
        w_own.start()
        o_own = local_copy(o_hbm.at[0], O.at[core])
        o_own.start()
        table_copy = local_copy(tables.at[:, pl.ds(pl.multiple_of(core * half, half), half)], TAB)
        table_copy.start()
        fresh_sem_all = fresh_sem("local", local_sem)
        fresh_rows = [
            pltpu.make_async_copy(fresh.at[core, :, span(c)], X.at[1, c, rows(own)], fresh_sem_all) for c in range(C)
        ]

        @pl.when(last)
        def _():
            SH[...] = jnp.zeros(SH.shape, SH.dtype)

        @pl.when(first)
        def _():
            for copy in fresh_rows:
                copy.start()

        barrier = pltpu.get_barrier_semaphore()
        for device in (dev_z, dev_up, dev_down, partner, ahead, behind):
            pl.semaphore_signal(barrier, inc=1, device_id=device, device_id_type=MESH)
        with jax.named_scope("entry"):
            pl.semaphore_wait(barrier, 6)
        for copy in small_loads:
            copy.wait()
        G[core] = jnp.broadcast_to(GIN[...].astype(jnp.float32), (8, gw))
        SEGS[0, core] = jnp.broadcast_to(SIN[...], (8, half))

        ag_sent = [send_group() for _ in range(2)]
        rs_sent = [send_group() for _ in range(2)]
        shift_sent = [send_group() for _ in range(2)]
        ag_sem = {(c, k): arrival() for c in range(C) for k in ("z", "y", "far", "rest")}
        rs_sem = {(c, k): arrival() for c in range(C) for k in ("q", "a", "z", "own")}

        ag = {}
        for l in range(2):
            for c in range(C):
                def block_of(b, device, kind, l=l, c=c):
                    ref = X.at[l, c, rows(b)]
                    return message(ref, ref, device, ag_sent[l], ag_sem[c, kind])
                even = c % 2 == 0
                ag[l, c] = dict(
                    z=block_of(own, dev_z, "z"),
                    down=block_of(own, dev_up, "y" if even else "rest"),
                    up=block_of(own, dev_down, "rest" if even else "y"),
                    z_down=block_of(rz, dev_up, "rest"),
                    z_up=block_of(rz, dev_down, "rest"),
                    far=block_of(down, dev_up, "far") if even else block_of(up, dev_down, "far"),
                    z_far=block_of(far, dev_z, "rest"),
                )

        def spread(l, c):
            for name in ("z", "down", "up"):
                ag[l, c][name].start()

        def relay_z(l, c):
            wait_for(X.at[l, c, rows(rz)], ag_sem[c, "z"])
            ag[l, c]["z_down"].start()
            ag[l, c]["z_up"].start()

        def relay_y(l, c):
            wait_for(X.at[l, c, rows(down if c % 2 == 0 else up)], ag_sem[c, "y"])
            ag[l, c]["far"].start()

        def relay_far(l, c):
            wait_for(X.at[l, c, rows(far)], ag_sem[c, "far"])
            ag[l, c]["z_far"].start()

        def gathered(l, c):
            wait_for(X.at[l, c, pl.ds(0, 4 * block)], ag_sem[c, "rest"])

        def spread_first(c):
            own_rows[c].wait()
            spread(0, c)

        w_sent = send_group()
        w_sem = [arrival() for _ in range(C)]
        small_sent, small_sem = [send_group() for _ in range(4)], [arrival() for _ in range(4)]
        w_other = {}
        for c in (c for k, c in FIRST_ORDER if k == 8):
            w_other[c] = message(w_hbm.at[:, span(c)], W.at[core, :, span(c)], partner, w_sent, w_sem[c])
            w_other[c].start()
            if len(w_other) == 1:
                gain_other = message(G.at[core], G.at[core], partner, small_sent[0], small_sem[0])
                gain_other.start()
                segments_other = message(
                    SEGS.at[0, core], SEGS.at[0, core], partner, small_sent[1], small_sem[1]
                )
                segments_other.start()
        o_other = message(o_hbm.at[0], O.at[core], partner, small_sent[2], small_sem[2])
        o_other.start()
        segments_ahead = message(SEGS.at[0], SEGS.at[1], ahead, small_sent[3], small_sem[3])

        begun = set()

        def multiply(l, c):
            opening = l not in begun
            begun.add(l)
            g0 = (c * cw) // gw
            scale = G[g0, 0:1, (c * cw) % gw:(c * cw) % gw + cw]

            def body(i, _):
                r = pl.ds(pl.multiple_of(i * 32, 32), 32)
                x = X[l, c, r].astype(jnp.float32)
                XG[r] = (x * scale).astype(jnp.bfloat16)
                square = x * x
                total = square[:, 0:HD]
                for k in range(1, cw // HD):
                    total = total + square[:, k * HD:(k + 1) * HD]
                if opening:
                    SS[r] = total
                else:
                    SS[r] = SS[r] + total
                return 0

            lax.fori_loop(0, half // 32, body, 0)
            for g in range(2):
                for j in range(3):
                    part = jnp.dot(XG[...], W[g, j, c * cw:(c + 1) * cw], preferred_element_type=jnp.float32)
                    if opening:
                        ACC[g, j] = part
                    else:
                        ACC[g, j] = ACC[g, j] + part

        def prepare(l):
            mine = jnp.broadcast_to(SEGS[l, core, 0:1], (HD, half)).astype(jnp.float32).T[:, 0:1]
            row_of = lax.broadcasted_iota(jnp.int32, (half, half), 0)
            column_of = lax.broadcasted_iota(jnp.int32, (half, half), 1)
            same = mine == SEGS[l, core, 0:1].astype(jnp.float32)
            BIAS[0] = jnp.where(same & (column_of <= row_of), 0.0, MASKED)
            BIAS[1] = jnp.where(mine == SEGS[l, 0, 0:1].astype(jnp.float32), 0.0, MASKED)

        def attend(l):
            power = jnp.sum(SS[...], axis=-1, keepdims=True) * (1.0 / width)
            factor = lax.rsqrt(power + EPS)
            heads = [(g, i) for g in range(2) for i in range(heads_each)]

            def rotated(v):
                return v * TAB[0] + pltpu.roll(v, HD // 2, 1) * TAB[1]

            values = message(KV.at[l, 1], KVO.at[l, 1], partner, send_group(), arrival())
            keys = message(KV.at[l, 0], KVO.at[l, 0], partner, send_group(), arrival())
            for h, (g, i) in enumerate(heads):
                KV[l, 0, h] = rotated(ACC[g, 1, :, i * HD:(i + 1) * HD] * factor).astype(jnp.bfloat16)

            @pl.when(core == 0)
            def _():
                keys.start()

            for h, (g, i) in enumerate(heads):
                KV[l, 1, h] = (ACC[g, 2, :, i * HD:(i + 1) * HD] * factor).astype(jnp.bfloat16)

            @pl.when(core == 0)
            def _():
                values.start()

            unsent_early.append(values)
            unsent_early.append(keys)
            for h, (g, i) in enumerate(heads):
                q = rotated(ACC[g, 0, :, i * HD:(i + 1) * HD] * factor).astype(jnp.bfloat16)
                MX[:, h * HD:(h + 1) * HD] = q
                scores = lax.dot_general(q, KV[l, 0, h], (((1,), (1,)), ((), ())), preferred_element_type=jnp.float32)
                near = scores * HD ** (-0.5) + BIAS[0]
                top = jnp.max(near, axis=-1, keepdims=True)
                near = jnp.exp(near - top)
                total = jnp.sum(near, axis=-1, keepdims=True)
                S[h, :, 0:HD] = jnp.broadcast_to(top, (half, HD))
                S[h, :, HD:2 * HD] = jnp.broadcast_to(total, (half, HD))
                S[h, :, 2 * HD:] = jnp.dot(near.astype(jnp.bfloat16), KV[l, 1, h], preferred_element_type=jnp.float32)

            def columns(h):
                return slice(h * HD, (h + 1) * HD)

            @pl.when(core == 0)
            def _():
                for h in range(len(heads)):
                    MX[:, columns(h)] = (S[h, :, 2 * HD:] / S[h, :, HD:2 * HD]).astype(jnp.bfloat16)

            @pl.when(core == 1)
            def _():
                with jax.named_scope("keys_wait"):
                    keys.wait_recv()
                for h in range(len(heads)):
                    away = lax.dot_general(
                        MX[:, columns(h)], KVO[l, 0, h], (((1,), (1,)), ((), ())), preferred_element_type=jnp.float32
                    )
                    away = away * HD ** (-0.5) + BIAS[1]
                    before = S[h, :, 0:HD]
                    top = jnp.maximum(before, jnp.max(away, axis=-1, keepdims=True))
                    kept = jnp.exp(before - top)
                    away = jnp.exp(away - top[:, 0:1])
                    if h == 0:
                        values.wait_recv()
                    total = S[h, :, HD:2 * HD] * kept + jnp.sum(away, axis=-1, keepdims=True)
                    mixed = S[h, :, 2 * HD:] * kept
                    mixed = mixed + jnp.dot(away.astype(jnp.bfloat16), KVO[l, 1, h], preferred_element_type=jnp.float32)
                    MX[:, columns(h)] = (mixed / total).astype(jnp.bfloat16)

        rs = {}
        for l in range(2):
            for c in range(C):
                def part(b, slot, device, kind, l=l, c=c):
                    return message(PB.at[l, c, rows(b)], R.at[l, c, slot], device, rs_sent[l], rs_sem[c, kind])
                even = c % 2 == 0
                rs[l, c] = dict(
                    b2=part(z_up, 2, dev_up, "z"),
                    b3=part(z_down, 3, dev_down, "z"),
                    b0=part(up, 4, dev_up, "own"),
                    b1=part(down, 5, dev_down, "own"),
                    z=part(rz, 6, dev_z, "own"),
                )
                if c in ALONG_Z[l]:
                    rs[l, c].update(q=part(z_far, 0, dev_z, "q"), a=part(far, 1, dev_up if even else dev_down, "a"))
                else:
                    rs[l, c].update(
                        a0=part(far if even else z_far, 0, dev_up, "q"), a1=part(z_far if even else far, 1, dev_down, "a")
                    )
        shift_sem = [[arrival() for _ in range(C)] for _ in range(2)]
        shifts = {}
        for c in range(C):
            shifts[0, c] = message(YS.at[0, c], X.at[1, c, rows(own)], ahead, shift_sent[0], shift_sem[0][c])
            shifts[1, c] = message(YS.at[1, c], SH.at[c], behind, shift_sent[1], shift_sem[1][c])

        def f32(v):
            return v.astype(jnp.float32)

        def project(l, c):
            PB[l, c] = jnp.dot(
                MX[...], O[:, :, c * cw:(c + 1) * cw].reshape(2 * cols, cw), preferred_element_type=jnp.float32
            ).astype(jnp.bfloat16)
            m = rs[l, c]
            for name in ("q", "b2", "b3") if c in ALONG_Z[l] else ("a0", "a1", "b2" if c % 2 == 0 else "b3"):
                m[name].start()

        def fold(l, c, slot, kind, b):
            wait_for(R.at[l, c, slot], rs_sem[c, kind])
            r = rows(b)
            PB[l, c, r] = (f32(PB[l, c, r]) + f32(R[l, c, slot])).astype(jnp.bfloat16)

        def fold_far(l, c):
            fold(l, c, 0, "q", far)
            rs[l, c]["a"].start()

        def fold_y(l, c):
            even = c % 2 == 0
            if c in ALONG_Z[l]:
                fold(l, c, 1, "a", up if even else down)
                return
            fold(l, c, 0, "q", up if even else z_up)
            fold(l, c, 1, "a", z_down if even else down)
            rs[l, c]["b3" if even else "b2"].start()

        def give(l, c):
            for name in ("b0", "b1"):
                rs[l, c][name].start()

        def fold_z(l, c):
            m = rs[l, c]
            wait_for(R.at[l, c, pl.ds(2, 2)], rs_sem[c, "z"])
            r = rows(rz)
            PB[l, c, r] = (f32(PB[l, c, r]) + f32(R[l, c, 2]) + f32(R[l, c, 3])).astype(jnp.bfloat16)
            m["z"].start()

        def finish(l, c):
            wait_for(R.at[l, c, pl.ds(4, 3)], rs_sem[c, "own"])
            r = rows(own)
            total = f32(PB[l, c, r]) + f32(R[l, c, 4]) + f32(R[l, c, 5]) + f32(R[l, c, 6])
            result = (f32(X[l, c, r]) + total).astype(jnp.bfloat16)
            YS[l, c] = result
            out[l, 0, :, c * cw:(c + 1) * cw] = result

            @pl.when(jnp.logical_not(last) if l == 0 else jnp.logical_not(first))
            def _():
                shifts[l, c].start()

        entered = []

        def enter(c):
            @pl.when(first)
            def _():
                if not entered:
                    wait_for(YS.at[0], fresh_sem_all)

            @pl.when(jnp.logical_not(first))
            def _():
                shifts[0, c].wait_recv()

            entered.append(c)
            spread(1, c)

        def leave(c):
            @pl.when(jnp.logical_not(last))
            def _():
                shifts[1, c].wait_recv()

            shadow[0, :, c * cw:(c + 1) * cw] = SH[c]

        def run(steps, order):
            for k, c in order:
                with jax.named_scope(f"step{k}c{c}"):
                    steps[k](c)

        gain_waited = []

        def compute_first(c):
            gathered(0, c)
            if not gain_waited:
                gain_other.wait_recv()
                gain_waited.append(True)
                w_own.wait()
                segments_other.wait_recv()

                @pl.when(jnp.logical_not(last))
                def _():
                    segments_ahead.start()

                prepare(0)
            w_other[c].wait_recv()
            multiply(0, c)

        run({
            4: spread_first,
            5: lambda c: relay_z(0, c),
            6: lambda c: relay_y(0, c),
            7: lambda c: relay_far(0, c),
            8: compute_first,
        }, FIRST_ORDER)
        table_copy.wait()
        with jax.named_scope("attend_first"):
            attend(0)
        o_own.wait()
        o_other.wait_recv()

        def segments_second():
            @pl.when(first)
            def _():
                for b in range(2):
                    SEGS[1, b] = jnp.broadcast_to(FIN[b:b + 1], (8, half))

            @pl.when(jnp.logical_not(first))
            def _():
                segments_ahead.wait_recv()
            prepare(1)

        def compute_second(c):
            if 1 not in begun:
                segments_second()
            gathered(1, c)
            multiply(1, c)

        run({
            0: lambda c: project(0, c),
            1: lambda c: fold_y(0, c),
            10: lambda c: fold_far(0, c),
            2: lambda c: fold_z(0, c),
            3: lambda c: finish(0, c),
            4: enter,
            5: lambda c: relay_z(1, c),
            6: lambda c: relay_y(1, c),
            7: lambda c: relay_far(1, c),
            8: compute_second,
            9: lambda c: give(0, c),
        }, MIDDLE_ORDER)

        with jax.named_scope("attend_second"):
            attend(1)
        run({
            0: lambda c: project(1, c),
            1: lambda c: fold_y(1, c),
            10: lambda c: fold_far(1, c),
            2: lambda c: fold_z(1, c),
            3: lambda c: finish(1, c),
            4: leave,
            9: lambda c: give(1, c),
        }, LAST_ORDER)
        with jax.named_scope("drain"):
            for l in range(2):
                wait_for(R.at[l], ag_sent[l])
                wait_for(R.at[l], rs_sent[l])
            wait_for(W.at[core], w_sent)
            for copy in (gain_other, segments_other, o_other):
                copy.wait_send()

        @pl.when(core == 0)
        def _():
            for copy in unsent_early:
                copy.wait_send()

        @pl.when(jnp.logical_not(last))
        def _():
            segments_ahead.wait_send()
            wait_for(YS.at[0], shift_sent[0])

        @pl.when(jnp.logical_not(first))
        def _():
            wait_for(YS.at[1], shift_sent[1])

    bf, f4 = jnp.bfloat16, jnp.float32
    heads = 2 * heads_each
    scratch = [
        pltpu.VMEM((2, C, half, cw), bf),
        pltpu.VMEM((2, 3, width, cols), bf),
        pltpu.VMEM((2, cols, width), bf),
        pltpu.VMEM((2, 3, half, cols), f4),
        pltpu.VMEM((half, HD), f4),
        pltpu.VMEM((half, cw), bf),
        pltpu.VMEM((2, C, half, cw), bf),
        pltpu.VMEM((2, C, 7, block, cw), bf),
        pltpu.VMEM((2, C, block, cw), bf),
        pltpu.VMEM((C, block, cw), bf),
        pltpu.VMEM((2, 2, heads, half, HD), bf),
        pltpu.VMEM((2, 2, heads, half, HD), bf),
        pltpu.VMEM((half, heads * HD), bf),
        pltpu.VMEM((heads, half, 3 * HD), f4),
        pltpu.VMEM((2, half, half), f4),
        pltpu.VMEM((2, 8, gw), f4),
        pltpu.VMEM((2, 2, 8, half), jnp.int32),
        pltpu.VMEM((2, half, HD), f4),
        pltpu.VMEM((1, gw), bf),
        pltpu.VMEM((1, half), jnp.int32),
        pltpu.VMEM((2, half), jnp.int32),
        pltpu.SemaphoreType.DMA((C + 7,)),
        pltpu.SemaphoreType.DMA((6 + 1 + 4 + 4,)),
        pltpu.SemaphoreType.DMA(((4 + 4 + 2 + 1) * C + 4 + 4,)),
    ]
    return kernel, scratch


def store(count):
    def kernel(*refs):
        sources, results, sem = refs[:count], refs[count:2 * count], refs[-1]
        for i in range(count):
            pltpu.make_async_copy(sources[i], results[i], sem.at[i]).start()
        for i in range(count):
            pltpu.make_async_copy(sources[i], results[i], sem.at[i]).wait()

    return kernel


def carry_over(arrays):
    hbm = pl.BlockSpec(memory_space=pl.ANY)
    vmem = pl.BlockSpec(memory_space=pltpu.VMEM)
    return pl.pallas_call(
        store(len(arrays)),
        name="store",
        out_shape=tuple(jax.ShapeDtypeStruct(a.shape, a.dtype) for a in arrays),
        in_specs=[vmem] * len(arrays),
        out_specs=(hbm,) * len(arrays),
        scratch_shapes=[pltpu.SemaphoreType.DMA((len(arrays),))],
        compiler_params=pltpu.CompilerParams(vmem_limit_bytes=2**20),
    )(*arrays)


def per_device(carried, carried_segments, fresh_batch, fresh_segments, qkv_weight, out_weight, norm_gain):
    _, block, width = carried.shape
    cols = qkv_weight.shape[-1]
    n_sections = lax.axis_size("section") // 2
    kernel, scratch = make_kernel(n_sections, width, block, cols // HD)
    weights = jnp.transpose(qkv_weight[0], (1, 0, 2))
    tables = jnp.asarray(rope_tables(16 * block))
    hbm = pl.BlockSpec(memory_space=pltpu.HBM)
    vmem = pl.BlockSpec(memory_space=pltpu.VMEM)
    out, shadow = pl.pallas_call(
        kernel,
        name="relay",
        out_shape=(
            pltpu.VMEM((2, 1, block, width), jnp.bfloat16),
            pltpu.VMEM((1, block, width), jnp.bfloat16),
        ),
        in_specs=[hbm] * 8,
        out_specs=(vmem, vmem),
        scratch_shapes=scratch,
        compiler_params=pltpu.CompilerParams(
            collective_id=0, has_side_effects=True, vmem_limit_bytes=60 * 2**20
        ),
    )(carried, carried_segments, fresh_batch, fresh_segments, weights, out_weight, norm_gain, tables)
    return carry_over((out, shadow))


def solution(mesh):
    return jax.shard_map(
        per_device,
        mesh=mesh,
        in_specs=(
            P("section", "tp", None),
            P("section", None),
            P(None, "tp", None),
            P(),
            P("section", None, None, "tp"),
            P("section", "tp", None),
            P("section", None),
        ),
        out_specs=(P(None, "section", "tp", None), P("section", "tp", None)),
        check_vma=False,
    )
```
